512 devices in a mesh: req: 16 (over y, core), seq: 32 (over z, x).
Axes of the slice: x: 4, y: 8, z: 8, core: 2. Of those that a mesh axis runs over, the one named last changes fastest.
Arguments:
- latent_cache: bfloat16 [16, 16384, 576], P('req', 'seq'), may hold values from -16 to 16
- queries: bfloat16 [16, 3, 128, 576], P('req', None, 'seq'), may hold values from -16 to 16
- chosen: int32 [16, 3, 32], P('req'), may hold values from 0 to 255, as said below
- position: int32 [16], P('req'), may hold values from 16321 to 16384
- w_value: bfloat16 [128, 512, 128], P('seq'), may hold values from -1.5 to 1.5
- w_out: bfloat16 [16384, 7168], P('seq', 'req'), may hold values from -0.09375 to 0.09375
Outputs:
- mixed_out: bfloat16 [7168, 48], P(('req', 'seq'))
The draws below stay inside these ranges and needn't reach their ends.
Inputs may be any that keep to these rules, and one draw needn't show every extreme that they name: `chosen`: block b holds positions b * 64 to b * 64 + 63, which lie on shard b // 8 of seq. A query's 32 numbers are distinct; at most 8 of them lie on one shard and exactly 8 on some shard, for every query; every query names the last block; its blocks on the other shards are spread as evenly as possible over those shards.
All inputs are finite; a program needn't handle non-finite values.
Results may differ from the reference program's by a relative error of at most 0.013.
Values may be sent and summed in bfloat16 or wider, within the bound.
No kernel may reach another device: no remote copies, remote signals or barrier semaphores. Data moves between devices by JAX's collectives and lax.ppermute only.
A program may use at most 128 MiB of HBM per device.

```python
import math
import jax
import jax.numpy as jnp
from jax import lax

HEADS = 128
LATENT = 512
ROPE = 64
VDIM = 128
D = 7168
BLOCK = 64
TOPB = 32
MAXB = 8
BLOCKS_DEV = 8
STEPS = 3
REQUESTS = 16
SEQLEN = 16384
N_SEQ = 32


def shuffled_row(row_key):
    return jax.random.permutation(row_key, BLOCKS_DEV).astype(jnp.int32)


def shuffled_short(row_key):
    return jax.random.permutation(row_key, BLOCKS_DEV - 1).astype(jnp.int32)


def one_query(key):
    others = TOPB - MAXB
    last_shard = N_SEQ - 1
    hot_shard = jax.random.randint(jax.random.fold_in(key, 1), (), 0, N_SEQ).astype(jnp.int32)
    spread_hot = jax.random.permutation(jax.random.fold_in(key, 2), BLOCKS_DEV)[:MAXB].astype(jnp.int32)
    tail_hot = jnp.concatenate([jnp.full((1,), BLOCKS_DEV - 1, jnp.int32), jax.random.permutation(jax.random.fold_in(key, 3), BLOCKS_DEV - 1)[:MAXB - 1].astype(jnp.int32)])
    hot_pick = jnp.where(hot_shard == last_shard, tail_hot, spread_hot)
    other_order = ((hot_shard + 1 + jax.random.permutation(jax.random.fold_in(key, 4), N_SEQ - 1)) % N_SEQ).astype(jnp.int32)
    leading = other_order[0]
    swapped = jnp.where(other_order == last_shard, leading, other_order)
    swapped = swapped.at[0].set(last_shard)
    other_order = jnp.where(hot_shard == last_shard, other_order, swapped)
    item_index = jnp.arange(others, dtype=jnp.int32)
    shard_ids = other_order[item_index % (N_SEQ - 1)]
    depth = item_index // (N_SEQ - 1)
    table_keys = jax.random.split(jax.random.fold_in(key, 5), N_SEQ)
    full_rows = jax.vmap(shuffled_row)(table_keys)
    tail_rows = jnp.concatenate([jnp.full((N_SEQ, 1), BLOCKS_DEV - 1, jnp.int32), jax.vmap(shuffled_short)(table_keys)], axis=1)
    row_is_last = (jnp.arange(N_SEQ, dtype=jnp.int32) == last_shard)[:, None]
    offsets_table = jnp.where(row_is_last, tail_rows, full_rows)
    other_blocks = shard_ids * BLOCKS_DEV + offsets_table[shard_ids, depth]
    blocks = jnp.concatenate([hot_shard * BLOCKS_DEV + hot_pick, other_blocks])
    return blocks[jax.random.permutation(jax.random.fold_in(key, 6), TOPB)]


def draw_chosen(key, part):
    query_keys = jax.random.split(jax.random.fold_in(key, 17), REQUESTS * STEPS)
    blocks = jax.vmap(one_query)(query_keys)
    return blocks.reshape(REQUESTS, STEPS, TOPB).astype(jnp.int32)


def draw_latent_cache(key, part):
    base = jax.random.fold_in(key, 31)
    shape = (REQUESTS, SEQLEN, LATENT + ROPE)
    values = jax.random.normal(base, shape, jnp.float32)
    return jnp.clip(values, -16.0, 16.0).astype(jnp.bfloat16)


def draw_queries(key, part):
    base = jax.random.fold_in(key, 47)
    shape = (REQUESTS, STEPS, HEADS, LATENT + ROPE)
    row_scale = jnp.exp(jax.random.uniform(jax.random.fold_in(key, 48), (REQUESTS, STEPS, HEADS, 1), jnp.float32, math.log(0.5), math.log(2.0)))
    values = jax.random.normal(base, shape, jnp.float32) * row_scale
    return jnp.clip(values, -16.0, 16.0).astype(jnp.bfloat16)


def set_ends(result, own_key, low, largest):
    longest = result.shape.index(max(result.shape))
    spots = []
    for shift in (0, 1):
        where = [jax.random.randint(jax.random.fold_in(own_key, axis), (), 0, length) for axis, length in enumerate(result.shape)]
        where[longest] = (where[longest] + shift) % result.shape[longest]
        spots.append(tuple(where))
    return result.at[spots[0]].set(low).at[spots[1]].set(largest)


def with_spikes(values, stream_key, source, target, parts, factor):
    def block_of(dim):
        return (jnp.arange(values.shape[dim]) // (values.shape[dim] // parts)).reshape((-1,) + (1,) * (values.ndim - 1 - dim))

    near = jax.random.permutation(stream_key, parts)[block_of(target)]
    far = (block_of(target) + parts // 2) % parts
    return jnp.where((block_of(source) == near) | (block_of(source) == far), factor * values, values)


def steps_of(key, shape, cuts, smallest, largest):
    def one(axis_at, parts):
        draws = jax.random.uniform(jax.random.fold_in(jax.random.fold_in(key, 6), axis_at), (parts,), jnp.float32, smallest / len(cuts), largest / len(cuts))
        return jnp.repeat(jnp.exp(draws), shape[axis_at] // parts).reshape((-1,) + (1,) * (len(shape) - axis_at - 1))

    level = one(*cuts[0])
    for cut in cuts[1:]:
        level = level * one(*cut)
    return level


def gaussian(stream_key, shape, width, bound, cuts=(), kind=jnp.bfloat16):
    drawn = width * jax.random.normal(stream_key, shape, jnp.float32)
    if cuts:
        drawn = drawn * steps_of(stream_key, shape, cuts, -0.22, 0.18)
    return jnp.clip(drawn, -bound, bound).astype(kind)


def noise_with(key, dims, width, most, pieces, heavy, held_as=jnp.bfloat16):
    array = width * jax.random.normal(key, dims, jnp.float32)
    if pieces:
        array = array * steps_of(key, dims, pieces, -0.22, 0.18)
    return jnp.clip(with_spikes(array, jax.random.fold_in(key, 3), *heavy), -most, most).astype(held_as)


def setup_inputs(seed: int = 0) -> dict:
    key_of = jax.random.split(jax.random.key(seed), 7)
    latent_cache = draw_latent_cache(jax.random.fold_in(key_of[6], 71), 0)
    queries = draw_queries(jax.random.fold_in(key_of[6], 71), 0)
    chosen = draw_chosen(jax.random.fold_in(key_of[6], 71), 0)
    position = set_ends(jax.random.randint(key_of[3], (REQUESTS,), SEQLEN - BLOCK + 1, SEQLEN + 1), jax.random.fold_in(key_of[3], 1), SEQLEN - BLOCK + 1, SEQLEN).astype(jnp.int32)
    w_value = gaussian(key_of[4], (HEADS, LATENT, VDIM), 16 ** -0.5, 1.5, ((0, 32),))
    w_out = noise_with(key_of[5], (HEADS * VDIM, D), (HEADS * VDIM) ** -0.5, 0.09375, ((0, 32), (1, 16)), (0, 1, 32, 2.75))
    return dict(latent_cache=latent_cache, queries=queries, chosen=chosen, position=position, w_value=w_value, w_out=w_out)


score_scale = 1.0 / math.sqrt(192.0)
very_low = -1e+30

def attend(query_rows, gathered, usable):
    query_wide = query_rows.astype(jnp.float32)
    gathered_wide = gathered.astype(jnp.float32)
    scores = jnp.dot(query_wide, gathered_wide.T, precision=lax.Precision.HIGHEST, preferred_element_type=jnp.float32) * score_scale
    scores = jnp.where(usable[None, :], scores, very_low)
    row_peak = lax.optimization_barrier(jnp.max(scores, axis=1, keepdims=True))
    raw_weights = jnp.where(usable[None, :], jnp.exp(scores - row_peak), 0.0)
    row_total = lax.optimization_barrier(jnp.sum(raw_weights, axis=1, keepdims=True))
    rounded = lax.optimization_barrier(raw_weights.astype(jnp.bfloat16))
    weighted = jnp.dot(rounded.astype(jnp.float32), gathered_wide[:, :LATENT], precision=lax.Precision.HIGHEST, preferred_element_type=jnp.float32)
    return (weighted / row_total).astype(jnp.bfloat16)

def reference(latent_cache, queries, chosen, position, w_value, w_out):
    inside = jnp.arange(BLOCK, dtype=jnp.int32)
    value_wide = w_value.astype(jnp.float32)

    def per_request(request):
        request_cache = latent_cache[request]
        per_step = []
        for decode_step in range(STEPS):
            token_ids = (chosen[request, decode_step][:, None] * BLOCK + inside[None, :]).reshape(-1)
            gathered = jnp.take(request_cache, token_ids, axis=0)
            usable = token_ids < position[request]
            latent_out = attend(queries[request, decode_step], gathered, usable)
            head_rows = jnp.einsum('hl,hlv->hv', latent_out.astype(jnp.float32), value_wide, precision=lax.Precision.HIGHEST).astype(jnp.bfloat16)
            per_step.append(head_rows.reshape(-1))
        return jnp.stack(per_step)
    head_out = lax.map(per_request, jnp.arange(REQUESTS, dtype=jnp.int32))
    head_out = lax.optimization_barrier(head_out)
    head_wide = head_out.reshape(REQUESTS * STEPS, HEADS * VDIM).astype(jnp.float32)
    mixed_out = jnp.dot(head_wide, w_out.astype(jnp.float32), precision=lax.Precision.HIGHEST, preferred_element_type=jnp.float32)
    return mixed_out.T.astype(jnp.bfloat16)
```

```python
import functools
import math

import jax
import jax.numpy as jnp
from jax import lax
from jax.experimental import pallas as pl
from jax.experimental.pallas import tpu as pltpu
from jax.sharding import PartitionSpec as P

LATENT = 512
BLOCK = 64
LANES = 128

score_scale = 1.0 / math.sqrt(192.0)
very_low = -1e30
f32 = jnp.float32
bf16 = jnp.bfloat16


def pieces(value):
    high = value.astype(bf16).astype(f32)
    rest = value - high
    middle = rest.astype(bf16).astype(f32)
    return high, middle, rest - middle


def attend_kernel(usable_ref, query_ref, cache_ref, out_ref, rows_ref, sums_ref):
    shards, steps, heads_dev, _ = query_ref.shape
    heads = shards * heads_dev
    for t in range(steps):
        for s in range(shards):
            rows_ref[t, s * heads_dev : (s + 1) * heads_dev, :] = query_ref[s, t]
    keys = cache_ref[...]
    latent = keys[:, :LATENT]
    lane = lax.broadcasted_iota(jnp.int32, (heads, LANES), 1)
    for t in range(steps):
        usable = usable_ref[t : t + 1, :] > 0.0
        scores = (
            lax.dot_general(
                rows_ref[t], keys, (((1,), (1,)), ((), ())), preferred_element_type=f32
            )
            * score_scale
        )
        scores = jnp.where(usable, scores, very_low)
        peak = jnp.max(scores, axis=1, keepdims=True)
        raw = jnp.where(usable, jnp.exp(scores - peak), 0.0)
        total = jnp.sum(raw, axis=1, keepdims=True)
        weighted = jnp.dot(raw.astype(bf16), latent, preferred_element_type=f32)
        sums_ref[t, :, :LATENT] = weighted.astype(bf16)
        stats = jnp.zeros((heads, LANES), f32)
        for k, piece in enumerate(pieces(peak) + pieces(total)):
            stats = jnp.where(lane == k, piece, stats)
        sums_ref[t, :, LATENT:] = stats.astype(bf16)
    for t in range(steps):
        for s in range(shards):
            out_ref[s, t] = sums_ref[t, s * heads_dev : (s + 1) * heads_dev, :]


def merge_kernel(parts_ref, value_ref, out_ref):
    shards, steps, heads_dev, _ = parts_ref.shape
    rows = []
    for t in range(steps):
        stats = parts_ref[:, t, :, LATENT:].astype(f32)
        peak = stats[:, :, 0:1] + stats[:, :, 1:2] + stats[:, :, 2:3]
        total = stats[:, :, 3:4] + stats[:, :, 4:5] + stats[:, :, 5:6]
        factor = jnp.exp(peak - jnp.max(peak, axis=0, keepdims=True))
        parts = parts_ref[:, t, :, :LATENT].astype(f32)
        latent_out = jnp.sum(parts * factor, axis=0) / jnp.sum(total * factor, axis=0)
        rows.append(latent_out.astype(bf16))
    row = lax.broadcasted_iota(jnp.int32, (heads_dev, value_ref.shape[2]), 0)
    for t in range(steps):
        for h in range(heads_dev):
            product = jnp.dot(rows[t], value_ref[h], preferred_element_type=f32)
            mine = jnp.sum(jnp.where(row == h, product, 0.0), axis=0, keepdims=True)
            width = value_ref.shape[2]
            out_ref[t : t + 1, h * width : (h + 1) * width] = mine.astype(bf16)


def exchanged(value, axis):
    return lax.all_to_all(value, axis, 0, 0, tiled=True)


def body(latent_cache, queries, chosen, position, w_value, w_out):
    cache_len, key_width = latent_cache.shape[1:]
    _, steps, heads_dev, _ = queries.shape
    shards = lax.axis_size("seq")
    requests = lax.axis_size("req")
    shard_index = lax.axis_index("seq")

    query_all = exchanged(
        jnp.broadcast_to(queries, (shards, steps, heads_dev, key_width)), "seq"
    )
    blocks = shard_index * (cache_len // BLOCK) + jnp.arange(cache_len, dtype=jnp.int32) // BLOCK
    rows = shard_index * cache_len + jnp.arange(cache_len, dtype=jnp.int32)
    usable = jnp.any(chosen[0][:, :, None] == blocks, axis=1) & (rows < position[0])
    message = LATENT + LANES
    parts = pl.pallas_call(
        attend_kernel,
        out_shape=jax.ShapeDtypeStruct((shards, steps, heads_dev, message), bf16),
        scratch_shapes=[
            pltpu.VMEM((steps, shards * heads_dev, key_width), bf16),
            pltpu.VMEM((steps, shards * heads_dev, message), bf16),
        ],
        name="attend",
    )(usable.astype(f32), query_all, latent_cache.reshape(cache_len, key_width))
    parts = exchanged(parts, "seq")
    vdim = w_value.shape[2]
    head_out = pl.pallas_call(
        merge_kernel,
        out_shape=jax.ShapeDtypeStruct((steps, heads_dev * vdim), bf16),
        name="merge",
    )(parts, w_value)
    every_request = exchanged(
        jnp.broadcast_to(head_out[None], (requests, *head_out.shape)), "req"
    )
    flat_heads = every_request.reshape(requests * steps, heads_dev * vdim)
    partial = lax.dot_general(
        w_out, flat_heads, (((0,), (1,)), ((), ())), preferred_element_type=f32
    ).astype(bf16)
    mixed = exchanged(partial.reshape(shards, 1, -1), "seq")
    mixed = jnp.sum(mixed.astype(f32), axis=0).astype(bf16)
    return mixed.reshape(-1, requests * steps)


def solution(mesh):
    return jax.shard_map(
        body,
        mesh=mesh,
        in_specs=(
            P("req", "seq", None),
            P("req", None, "seq", None),
            P("req", None, None),
            P("req"),
            P("seq", None, None),
            P("seq", "req"),
        ),
        out_specs=P(("req", "seq"), None),
        check_vma=False,
    )
```

```python
import math

import jax
import jax.numpy as jnp
from jax import lax
from jax.experimental import pallas as pl
from jax.experimental.pallas import tpu as pltpu
from jax.sharding import PartitionSpec as P

LATENT = 512
ROPE = 64
BLOCK = 64
LANES = 128
CHUNKS = LATENT // LANES
GRANT = 12 * 1024 * 1024

score_scale = 1.0 / math.sqrt(192.0)
very_low = -1e30
f32 = jnp.float32
bf16 = jnp.bfloat16


def pieces(value):
    high = value.astype(bf16).astype(f32)
    rest = value - high
    middle = rest.astype(bf16).astype(f32)
    return high, middle, rest - middle


def spread_kernel(query_ref, out_ref):
    steps, heads_dev, _ = query_ref.shape
    packed = []
    for t in range(steps):
        for c in range(CHUNKS):
            packed.append(query_ref[t, :, c * LANES : (c + 1) * LANES])
    rotary = [query_ref[t, :, LATENT:] for t in range(steps)]
    rotary.append(jnp.zeros_like(rotary[0]))
    for t in range(0, len(rotary), 2):
        packed.append(jnp.concatenate([rotary[t], rotary[t + 1]], axis=1))
    for k, piece in enumerate(packed):
        out_ref[:, k * heads_dev : (k + 1) * heads_dev, :] = jnp.broadcast_to(
            piece[None], (out_ref.shape[0], heads_dev, LANES)
        )


def attend_kernel(usable_ref, query_ref, cache_ref, out_ref, rows_ref, rotary_ref, sums_ref):
    shards = query_ref.shape[0]
    steps, heads, _ = rows_ref.shape
    heads_dev = heads // shards
    for s in range(shards):
        span = slice(s * heads_dev, (s + 1) * heads_dev)
        for t in range(steps):
            for c in range(CHUNKS):
                k = (t * CHUNKS + c) * heads_dev
                rows_ref[t, span, c * LANES : (c + 1) * LANES] = query_ref[s, k : k + heads_dev, :]
        for pair in range(rotary_ref.shape[0]):
            k = (steps * CHUNKS + pair) * heads_dev
            rotary_ref[pair, span, :] = query_ref[s, k : k + heads_dev, :]
    latent = cache_ref[:LATENT, :]
    rotary_keys = cache_ref[LATENT:, :]
    lane = lax.broadcasted_iota(jnp.int32, (heads, LANES), 1)
    stats = jnp.zeros((heads, LANES), f32)
    for t in range(steps):
        usable = usable_ref[t : t + 1, :] > 0.0
        rotary = rotary_ref[t // 2, :, (t % 2) * ROPE : (t % 2 + 1) * ROPE]
        scores = jnp.dot(rows_ref[t], latent, preferred_element_type=f32)
        scores = scores + jnp.dot(rotary, rotary_keys, preferred_element_type=f32)
        scores = jnp.where(usable, scores * score_scale, very_low)
        peak = jnp.max(scores, axis=1, keepdims=True)
        raw = jnp.where(usable, jnp.exp(scores - peak), 0.0)
        total = jnp.sum(raw, axis=1, keepdims=True)
        weighted = lax.dot_general(
            raw.astype(bf16), latent, (((1,), (1,)), ((), ())), preferred_element_type=f32
        )
        sums_ref[:, t * LATENT : (t + 1) * LATENT] = weighted.astype(bf16)
        for k, piece in enumerate(pieces(peak) + pieces(total)):
            stats = jnp.where(lane == t * 6 + k, piece, stats)
    sums_ref[:, steps * LATENT :] = stats.astype(bf16)
    for s in range(shards):
        for k in range(out_ref.shape[1]):
            out_ref[s, k] = sums_ref[
                s * heads_dev : (s + 1) * heads_dev, k * LANES : (k + 1) * LANES
            ]


def merge_kernel(parts_ref, value_ref, out_ref):
    shards, _, heads_dev, _ = parts_ref.shape
    requests, steps, _, _ = out_ref.shape
    stats = parts_ref[:, steps * CHUNKS].astype(f32)
    row = lax.broadcasted_iota(jnp.int32, (heads_dev, LANES), 0)
    for t in range(steps):
        k = t * 6
        peak = stats[:, :, k : k + 1] + stats[:, :, k + 1 : k + 2] + stats[:, :, k + 2 : k + 3]
        total = stats[:, :, k + 3 : k + 4] + stats[:, :, k + 4 : k + 5] + stats[:, :, k + 5 : k + 6]
        factor = jnp.exp(peak - jnp.max(peak, axis=0, keepdims=True))
        whole = jnp.sum(total * factor, axis=0)
        wide = jnp.broadcast_to(factor, (shards, heads_dev, LANES))
        latent_out = []
        for c in range(CHUNKS):
            part = parts_ref[:, t * CHUNKS + c].astype(f32)
            latent_out.append((jnp.sum(part * wide, axis=0) / whole).astype(bf16))
        latent_out = jnp.concatenate(latent_out, axis=1)
        heads = jnp.zeros((heads_dev, LANES), f32)
        for h in range(heads_dev):
            product = jnp.dot(latent_out, value_ref[h], preferred_element_type=f32)
            heads = jnp.where(row == h, product, heads)
        out_ref[:, t] = jnp.broadcast_to(heads.astype(bf16)[None], (requests, heads_dev, LANES))


def project_kernel(heads_ref, weight_ref, out_ref, flat_ref, wide_ref):
    requests, steps, heads_dev, _ = heads_ref.shape
    queries = requests * steps
    shards, half, width = out_ref.shape
    for q in range(queries):
        flat_ref[q * heads_dev : (q + 1) * heads_dev, :] = heads_ref[q // steps, q % steps]
    every = flat_ref[...]
    out_row = lax.broadcasted_iota(jnp.int32, (width, queries * heads_dev), 0)
    in_row = lax.broadcasted_iota(jnp.int32, (width, queries * heads_dev), 1)
    source = jnp.where(out_row < queries, out_row, out_row - queries) * heads_dev
    mixed = jnp.zeros(wide_ref.shape, f32)
    for h in range(heads_dev):
        pick = jnp.where(in_row == source + h, 1.0, 0.0).astype(bf16)
        of_head = jnp.dot(pick, every, preferred_element_type=f32).astype(bf16)
        mixed = mixed + lax.dot_general(
            weight_ref[:, h * LANES : (h + 1) * LANES],
            of_head,
            (((1,), (1,)), ((), ())),
            preferred_element_type=f32,
        )
    wide_ref[...] = mixed
    lane = lax.broadcasted_iota(jnp.int32, (half, width), 1)
    for s in range(shards):
        first = wide_ref[2 * half * s : 2 * half * s + half, :]
        second = wide_ref[2 * half * s + half : 2 * half * (s + 1), :]
        out_ref[s] = jnp.where(lane < queries, first, second).astype(bf16)


def finish_kernel(parts_ref, out_ref):
    _, half, width = parts_ref.shape
    total = jnp.sum(parts_ref[...].astype(f32), axis=0)
    out_ref[:half, :] = total[:, : width // 2].astype(bf16)
    out_ref[half:, :] = total[:, width // 2 :].astype(bf16)


def exchanged(value, axis):
    return lax.all_to_all(value, axis, 0, 0, tiled=True)


def kernel(fn, shape, name, scratch=(), dtype=bf16):
    return pl.pallas_call(
        fn,
        out_shape=jax.ShapeDtypeStruct(shape, dtype),
        scratch_shapes=[pltpu.VMEM(*s) for s in scratch],
        compiler_params=pltpu.CompilerParams(vmem_limit_bytes=GRANT),
        name=name,
    )


def body(latent_cache, queries, chosen, position, w_value, w_out):
    cache_len, key_width = latent_cache.shape[1:]
    _, steps, heads_dev, _ = queries.shape
    shards = lax.axis_size("seq")
    requests = lax.axis_size("req")
    shard_index = lax.axis_index("seq")
    heads = shards * heads_dev

    packed_rows = (steps * CHUNKS + (steps + 1) // 2) * heads_dev
    query_all = kernel(spread_kernel, (shards, packed_rows, LANES), "spread")(queries[0])
    query_all = exchanged(query_all, "seq")

    rows = shard_index * cache_len + jnp.arange(cache_len, dtype=jnp.int32)
    usable = jnp.any(chosen[0][:, :, None] == rows // BLOCK, axis=1) & (rows < position[0])
    parts = kernel(
        attend_kernel,
        (shards, steps * CHUNKS + 1, heads_dev, LANES),
        "attend",
        (
            ((steps, heads, LATENT), bf16),
            (((steps + 1) // 2, heads, LANES), bf16),
            ((heads, steps * LATENT + LANES), bf16),
        ),
    )(usable.astype(f32), query_all, latent_cache[0].T)
    parts = exchanged(parts, "seq")
    head_out = kernel(merge_kernel, (requests, steps, heads_dev, w_value.shape[2]), "merge")(
        parts, w_value
    )
    head_out = exchanged(head_out, "req")
    features = w_out.shape[1]
    count = requests * steps
    mixed = kernel(
        project_kernel,
        (shards, features // shards // 2, 2 * count),
        "project",
        (((count * heads_dev, LANES), bf16), ((features, 2 * count), f32)),
    )(head_out, w_out.T)
    mixed = exchanged(mixed, "seq")
    return kernel(finish_kernel, (features // shards, count), "finish")(mixed)


def solution(mesh):
    return jax.shard_map(
        body,
        mesh=mesh,
        in_specs=(
            P("req", "seq", None),
            P("req", None, "seq", None),
            P("req", None, None),
            P("req"),
            P("seq", None, None),
            P("seq", "req"),
        ),
        out_specs=P(("req", "seq"), None),
        check_vma=False,
    )
```

```python
import math

import jax
import jax.numpy as jnp
from jax import lax
from jax.experimental import pallas as pl
from jax.experimental.pallas import tpu as pltpu
from jax.sharding import PartitionSpec as P

LATENT = 512
ROPE = 64
BLOCK = 64
LANES = 128
CHUNKS = LATENT // LANES
GRANT = 12 * 1024 * 1024

score_scale = 1.0 / math.sqrt(192.0)
very_low = -1e30
f32 = jnp.float32
bf16 = jnp.bfloat16


def pieces(value):
    high = value.astype(bf16).astype(f32)
    rest = value - high
    middle = rest.astype(bf16).astype(f32)
    return high, middle, rest - middle


def spread_kernel(query_hbm, chosen_hbm, position_ref, out_ref, usable_ref, query_ref, chosen_ref, sems):
    copies = [
        pltpu.make_async_copy(source, target, sems.at[k])
        for k, (source, target) in enumerate(
            ((query_hbm, query_ref), (chosen_hbm, chosen_ref))
        )
    ]
    for copy in copies:
        copy.start()
    for copy in copies:
        copy.wait()
    steps, heads_dev, _ = query_ref.shape
    packed = []
    for t in range(steps):
        for c in range(CHUNKS):
            packed.append(query_ref[t, :, c * LANES : (c + 1) * LANES])
    rotary = [query_ref[t, :, LATENT:] for t in range(steps)]
    rotary.append(jnp.zeros_like(rotary[0]))
    for t in range(0, len(rotary), 2):
        packed.append(jnp.concatenate([rotary[t], rotary[t + 1]], axis=1))
    for k, piece in enumerate(packed):
        out_ref[:, k * heads_dev : (k + 1) * heads_dev, :] = jnp.broadcast_to(
            piece[None], (out_ref.shape[0], heads_dev, LANES)
        )
    cache_len = usable_ref.shape[1]
    row = lax.axis_index("seq") * cache_len + lax.broadcasted_iota(jnp.int32, (1, cache_len), 1)
    block = row // BLOCK
    inside = row < position_ref[0]
    for t in range(steps):
        named = jnp.zeros((1, cache_len), jnp.bool_)
        for k in range(chosen_ref.shape[2]):
            named = named | (block == chosen_ref[t, :, k : k + 1])
        usable_ref[t : t + 1, :] = jnp.where(named & inside, 1.0, 0.0)


def attend_kernel(usable_ref, query_ref, cache_ref, out_ref, rows_ref, rotary_ref, sums_ref):
    shards = query_ref.shape[0]
    steps, heads, _ = rows_ref.shape
    heads_dev = heads // shards
    for s in range(shards):
        span = slice(s * heads_dev, (s + 1) * heads_dev)
        for t in range(steps):
            for c in range(CHUNKS):
                k = (t * CHUNKS + c) * heads_dev
                rows_ref[t, span, c * LANES : (c + 1) * LANES] = query_ref[s, k : k + heads_dev, :]
        for pair in range(rotary_ref.shape[0]):
            k = (steps * CHUNKS + pair) * heads_dev
            rotary_ref[pair, span, :] = query_ref[s, k : k + heads_dev, :]
    latent = cache_ref[:LATENT, :]
    rotary_keys = cache_ref[LATENT:, :]
    lane = lax.broadcasted_iota(jnp.int32, (heads, LANES), 1)
    stats = jnp.zeros((heads, LANES), f32)
    for t in range(steps):
        usable = usable_ref[t : t + 1, :] > 0.0
        rotary = rotary_ref[t // 2, :, (t % 2) * ROPE : (t % 2 + 1) * ROPE]
        scores = jnp.dot(rows_ref[t], latent, preferred_element_type=f32)
        scores = scores + jnp.dot(rotary, rotary_keys, preferred_element_type=f32)
        scores = jnp.where(usable, scores * score_scale, very_low)
        peak = jnp.max(scores, axis=1, keepdims=True)
        raw = jnp.where(usable, jnp.exp(scores - peak), 0.0)
        total = jnp.sum(raw, axis=1, keepdims=True)
        weighted = lax.dot_general(
            raw.astype(bf16), latent, (((1,), (1,)), ((), ())), preferred_element_type=f32
        )
        sums_ref[:, t * LATENT : (t + 1) * LATENT] = weighted.astype(bf16)
        for k, piece in enumerate(pieces(peak) + pieces(total)):
            stats = jnp.where(lane == t * 6 + k, piece, stats)
    sums_ref[:, steps * LATENT :] = stats.astype(bf16)
    for s in range(shards):
        for k in range(out_ref.shape[1]):
            out_ref[s, k] = sums_ref[
                s * heads_dev : (s + 1) * heads_dev, k * LANES : (k + 1) * LANES
            ]


def merge_kernel(parts_ref, value_ref, out_ref):
    shards, _, heads_dev, _ = parts_ref.shape
    requests, steps, _, _ = out_ref.shape
    stats = parts_ref[:, steps * CHUNKS].astype(f32)
    row = lax.broadcasted_iota(jnp.int32, (heads_dev, LANES), 0)
    for t in range(steps):
        k = t * 6
        peak = stats[:, :, k : k + 1] + stats[:, :, k + 1 : k + 2] + stats[:, :, k + 2 : k + 3]
        total = stats[:, :, k + 3 : k + 4] + stats[:, :, k + 4 : k + 5] + stats[:, :, k + 5 : k + 6]
        factor = jnp.exp(peak - jnp.max(peak, axis=0, keepdims=True))
        whole = jnp.sum(total * factor, axis=0)
        wide = jnp.broadcast_to(factor, (shards, heads_dev, LANES))
        latent_out = []
        for c in range(CHUNKS):
            part = parts_ref[:, t * CHUNKS + c].astype(f32)
            latent_out.append((jnp.sum(part * wide, axis=0) / whole).astype(bf16))
        latent_out = jnp.concatenate(latent_out, axis=1)
        heads = jnp.zeros((heads_dev, LANES), f32)
        for h in range(heads_dev):
            product = jnp.dot(latent_out, value_ref[h], preferred_element_type=f32)
            heads = jnp.where(row == h, product, heads)
        out_ref[:, t] = jnp.broadcast_to(heads.astype(bf16)[None], (requests, heads_dev, LANES))


def project_kernel(heads_ref, weight_ref, out_ref, flat_ref, wide_ref):
    requests, steps, heads_dev, _ = heads_ref.shape
    queries = requests * steps
    shards, half, width = out_ref.shape
    for q in range(queries):
        flat_ref[q * heads_dev : (q + 1) * heads_dev, :] = heads_ref[q // steps, q % steps]
    every = flat_ref[...]
    out_row = lax.broadcasted_iota(jnp.int32, (width, queries * heads_dev), 0)
    in_row = lax.broadcasted_iota(jnp.int32, (width, queries * heads_dev), 1)
    source = jnp.where(out_row < queries, out_row, out_row - queries) * heads_dev
    mixed = jnp.zeros(wide_ref.shape, f32)
    for h in range(heads_dev):
        pick = jnp.where(in_row == source + h, 1.0, 0.0).astype(bf16)
        of_head = jnp.dot(pick, every, preferred_element_type=f32).astype(bf16)
        mixed = mixed + lax.dot_general(
            weight_ref[:, h * LANES : (h + 1) * LANES],
            of_head,
            (((1,), (1,)), ((), ())),
            preferred_element_type=f32,
        )
    wide_ref[...] = mixed
    lane = lax.broadcasted_iota(jnp.int32, (half, width), 1)
    for s in range(shards):
        first = wide_ref[2 * half * s : 2 * half * s + half, :]
        second = wide_ref[2 * half * s + half : 2 * half * (s + 1), :]
        out_ref[s] = jnp.where(lane < queries, first, second).astype(bf16)


def finish_kernel(parts_ref, out_ref):
    _, half, width = parts_ref.shape
    total = jnp.sum(parts_ref[...].astype(f32), axis=0)
    out_ref[:half, :] = total[:, : width // 2].astype(bf16)
    out_ref[half:, :] = total[:, width // 2 :].astype(bf16)


def exchanged(value, axis):
    return lax.all_to_all(value, axis, 0, 0, tiled=True)


def kernel(fn, shape, name, scratch=(), dtype=bf16):
    return pl.pallas_call(
        fn,
        out_shape=jax.ShapeDtypeStruct(shape, dtype),
        scratch_shapes=[pltpu.VMEM(*s) for s in scratch],
        compiler_params=pltpu.CompilerParams(vmem_limit_bytes=GRANT),
        name=name,
    )


def body(latent_cache, queries, chosen, position, w_value, w_out):
    cache_len, key_width = latent_cache.shape[1:]
    _, steps, heads_dev, _ = queries.shape
    shards = lax.axis_size("seq")
    requests = lax.axis_size("req")
    heads = shards * heads_dev

    packed_rows = (steps * CHUNKS + (steps + 1) // 2) * heads_dev
    query_all, usable = pl.pallas_call(
        spread_kernel,
        out_shape=(
            jax.ShapeDtypeStruct((shards, packed_rows, LANES), bf16),
            jax.ShapeDtypeStruct((steps, cache_len), f32),
        ),
        in_specs=[pl.BlockSpec(memory_space=pltpu.HBM)] * 2
        + [pl.BlockSpec(memory_space=pltpu.SMEM)],
        scratch_shapes=[
            pltpu.VMEM((steps, heads_dev, key_width), bf16),
            pltpu.VMEM((steps, 1, chosen.shape[2]), jnp.int32),
            pltpu.SemaphoreType.DMA((2,)),
        ],
        compiler_params=pltpu.CompilerParams(vmem_limit_bytes=GRANT),
        name="spread",
    )(
        pltpu.with_memory_space_constraint(queries[0], pltpu.HBM),
        pltpu.with_memory_space_constraint(jnp.swapaxes(chosen, 0, 1), pltpu.HBM),
        position,
    )
    query_all = exchanged(query_all, "seq")
    parts = kernel(
        attend_kernel,
        (shards, steps * CHUNKS + 1, heads_dev, LANES),
        "attend",
        (
            ((steps, heads, LATENT), bf16),
            (((steps + 1) // 2, heads, LANES), bf16),
            ((heads, steps * LATENT + LANES), bf16),
        ),
    )(usable, query_all, latent_cache[0].T)
    parts = exchanged(parts, "seq")
    head_out = kernel(merge_kernel, (requests, steps, heads_dev, w_value.shape[2]), "merge")(
        parts, w_value
    )
    head_out = exchanged(head_out, "req")
    features = w_out.shape[1]
    count = requests * steps
    mixed = kernel(
        project_kernel,
        (shards, features // shards // 2, 2 * count),
        "project",
        (((count * heads_dev, LANES), bf16), ((features, 2 * count), f32)),
    )(head_out, w_out.T)
    mixed = exchanged(mixed, "seq")
    return kernel(finish_kernel, (features // shards, count), "finish")(mixed)


def solution(mesh):
    return jax.shard_map(
        body,
        mesh=mesh,
        in_specs=(
            P("req", "seq", None),
            P("req", None, "seq", None),
            P("req", None, None),
            P("req"),
            P("seq", None, None),
            P("seq", "req"),
        ),
        out_specs=P(("req", "seq"), None),
        check_vma=False,
    )
```

```python
import math

import jax
import jax.numpy as jnp
from jax import lax
from jax.experimental import pallas as pl
from jax.experimental.pallas import tpu as pltpu
from jax.sharding import PartitionSpec as P

LATENT = 512
ROPE = 64
BLOCK = 64
LANES = 128
CHUNKS = LATENT // LANES
GRANT = 12 * 1024 * 1024

score_scale = 1.0 / math.sqrt(192.0)
very_low = -1e30
f32 = jnp.float32
bf16 = jnp.bfloat16


def pieces(value):
    high = value.astype(bf16).astype(f32)
    rest = value - high
    middle = rest.astype(bf16).astype(f32)
    return high, middle, rest - middle


def spread_kernel(query_hbm, chosen_hbm, position_ref, out_ref, usable_ref, query_ref, chosen_ref, sems):
    copies = [
        pltpu.make_async_copy(source, target, sems.at[k])
        for k, (source, target) in enumerate(
            ((query_hbm, query_ref), (chosen_hbm, chosen_ref))
        )
    ]
    for copy in copies:
        copy.start()
    for copy in copies:
        copy.wait()
    steps, heads_dev, _ = query_ref.shape
    packed = []
    for t in range(steps):
        for c in range(CHUNKS):
            packed.append(query_ref[t, :, c * LANES : (c + 1) * LANES])
    rotary = [query_ref[t, :, LATENT:] for t in range(steps)]
    rotary.append(jnp.zeros_like(rotary[0]))
    for t in range(0, len(rotary), 2):
        packed.append(jnp.concatenate([rotary[t], rotary[t + 1]], axis=1))
    for k, piece in enumerate(packed):
        out_ref[:, k * heads_dev : (k + 1) * heads_dev, :] = jnp.broadcast_to(
            piece[None], (out_ref.shape[0], heads_dev, LANES)
        )
    cache_len = usable_ref.shape[1]
    blocks = cache_len // BLOCK
    first = lax.axis_index("seq") * cache_len
    column = lax.broadcasted_iota(jnp.int32, (blocks, cache_len), 1)
    mine = column // BLOCK == lax.broadcasted_iota(jnp.int32, (blocks, cache_len), 0)
    mine = mine & (first + column < position_ref[0])
    wanted = chosen_ref.shape[2]
    block = first // BLOCK + lax.broadcasted_iota(jnp.int32, (blocks, wanted), 0)
    for t in range(steps):
        named = jnp.where(chosen_ref[t] == block, 1.0, 0.0)
        named = jnp.max(named, axis=1, keepdims=True)
        usable_ref[t : t + 1, :] = jnp.max(jnp.where(mine, named, 0.0), axis=0, keepdims=True)


def attend_kernel(usable_ref, query_ref, cache_ref, out_ref, rotary_ref, stats_ref, *work):
    shards = query_ref.shape[0]
    steps = usable_ref.shape[0]
    heads = rotary_ref.shape[1]
    heads_dev = heads // shards
    spans = [slice(s * heads_dev, (s + 1) * heads_dev) for s in range(shards)]
    for pair in range(rotary_ref.shape[0]):
        k = (steps * CHUNKS + pair) * heads_dev
        for s in range(shards):
            rotary_ref[pair, spans[s], :] = query_ref[s, k : k + heads_dev, :]
    latent = cache_ref[:LATENT, :]
    rotary_keys = cache_ref[LATENT:, :]
    lane = lax.broadcasted_iota(jnp.int32, (heads, LANES), 1)
    slot = lane % (2 * steps)
    stats = jnp.zeros((heads, LANES), f32)
    for t in range(steps):
        rows_ref, sums_ref = work[2 * t], work[2 * t + 1]
        for c in range(CHUNKS):
            k = (t * CHUNKS + c) * heads_dev
            for s in range(shards):
                rows_ref[spans[s], c * LANES : (c + 1) * LANES] = query_ref[s, k : k + heads_dev, :]
        rotary = rotary_ref[t // 2, :, (t % 2) * ROPE : (t % 2 + 1) * ROPE]
        scores = jnp.dot(rows_ref[...], latent, preferred_element_type=f32)
        scores = scores + jnp.dot(rotary, rotary_keys, preferred_element_type=f32)
        scores = jnp.where(usable_ref[t : t + 1, :] > 0.0, scores, very_low)
        peak = jnp.max(scores, axis=1, keepdims=True)
        raw = jnp.exp2((scores - peak) * (score_scale * math.log2(math.e)))
        total = jnp.sum(raw, axis=1, keepdims=True)
        sums_ref[...] = lax.dot_general(
            raw.astype(bf16), latent, (((1,), (1,)), ((), ())), preferred_element_type=f32
        ).astype(bf16)
        stats = jnp.where(slot == 2 * t, peak * score_scale, stats)
        stats = jnp.where(slot == 2 * t + 1, total, stats)
        for c in range(CHUNKS):
            for s in range(shards):
                out_ref[s, t * CHUNKS + c] = sums_ref[spans[s], c * LANES : (c + 1) * LANES]
    high, middle, low = pieces(stats)
    stats = jnp.where(lane < 2 * steps, high, jnp.where(lane < 4 * steps, middle, low))
    stats_ref[...] = stats.astype(bf16)
    for s in range(shards):
        out_ref[s, steps * CHUNKS] = stats_ref[spans[s], :]


def merge_kernel(parts_ref, value_ref, out_ref):
    shards, _, heads_dev, _ = parts_ref.shape
    requests, steps, _, _ = out_ref.shape
    stats = parts_ref[:, steps * CHUNKS].astype(f32)
    latent_out = []
    for t in range(steps):
        peak, total = (
            stats[:, :, k : k + 1]
            + stats[:, :, k + 2 * steps : k + 2 * steps + 1]
            + stats[:, :, k + 4 * steps : k + 4 * steps + 1]
            for k in (2 * t, 2 * t + 1)
        )
        factor = jnp.exp(peak - jnp.max(peak, axis=0, keepdims=True))
        whole = jnp.sum(total * factor, axis=0)
        wide = jnp.broadcast_to(factor, (shards, heads_dev, LANES))
        chunks = []
        for c in range(CHUNKS):
            part = parts_ref[:, t * CHUNKS + c].astype(f32)
            chunks.append(jnp.sum(part * wide, axis=0) / whole)
        latent_out.append(jnp.concatenate(chunks, axis=1))
    latent_out = jnp.concatenate(latent_out, axis=0).astype(bf16)
    row = lax.broadcasted_iota(jnp.int32, (steps * heads_dev, LANES), 0) % heads_dev
    heads = jnp.zeros((steps * heads_dev, LANES), f32)
    for h in range(heads_dev):
        product = jnp.dot(latent_out, value_ref[h], preferred_element_type=f32)
        heads = jnp.where(row == h, product, heads)
    for t in range(steps):
        mine = heads[t * heads_dev : (t + 1) * heads_dev, :].astype(bf16)
        out_ref[:, t] = jnp.broadcast_to(mine[None], (requests, heads_dev, LANES))


def project_kernel(heads_ref, weight_ref, out_ref, flat_ref, wide_ref):
    requests, steps, heads_dev, _ = heads_ref.shape
    queries = requests * steps
    shards, half, width = out_ref.shape
    for q in range(queries):
        flat_ref[q * heads_dev : (q + 1) * heads_dev, :] = heads_ref[q // steps, q % steps]
    every = flat_ref[...]
    out_row = lax.broadcasted_iota(jnp.int32, (width, queries * heads_dev), 0)
    in_row = lax.broadcasted_iota(jnp.int32, (width, queries * heads_dev), 1)
    source = jnp.where(out_row < queries, out_row, out_row - queries) * heads_dev
    mixed = jnp.zeros(wide_ref.shape, f32)
    for h in range(heads_dev):
        pick = jnp.where(in_row == source + h, 1.0, 0.0).astype(bf16)
        of_head = jnp.dot(pick, every, preferred_element_type=f32).astype(bf16)
        mixed = mixed + lax.dot_general(
            weight_ref[:, h * LANES : (h + 1) * LANES],
            of_head,
            (((1,), (1,)), ((), ())),
            preferred_element_type=f32,
        )
    wide_ref[...] = mixed
    lane = lax.broadcasted_iota(jnp.int32, (half, width), 1)
    for s in range(shards):
        first = wide_ref[2 * half * s : 2 * half * s + half, :]
        second = wide_ref[2 * half * s + half : 2 * half * (s + 1), :]
        out_ref[s] = jnp.where(lane < queries, first, second).astype(bf16)


def finish_kernel(parts_ref, out_ref):
    _, half, width = parts_ref.shape
    total = jnp.sum(parts_ref[...].astype(f32), axis=0)
    out_ref[:half, :] = total[:, : width // 2].astype(bf16)
    out_ref[half:, :] = total[:, width // 2 :].astype(bf16)


def exchanged(value, axis):
    return lax.all_to_all(value, axis, 0, 0, tiled=True)


def kernel(fn, shape, name, scratch=(), dtype=bf16):
    return pl.pallas_call(
        fn,
        out_shape=jax.ShapeDtypeStruct(shape, dtype),
        scratch_shapes=[pltpu.VMEM(*s) for s in scratch],
        compiler_params=pltpu.CompilerParams(vmem_limit_bytes=GRANT),
        name=name,
    )


def body(latent_cache, queries, chosen, position, w_value, w_out):
    cache_len, key_width = latent_cache.shape[1:]
    _, steps, heads_dev, _ = queries.shape
    shards = lax.axis_size("seq")
    requests = lax.axis_size("req")
    heads = shards * heads_dev

    packed_rows = (steps * CHUNKS + (steps + 1) // 2) * heads_dev
    query_all, usable = pl.pallas_call(
        spread_kernel,
        out_shape=(
            jax.ShapeDtypeStruct((shards, packed_rows, LANES), bf16),
            jax.ShapeDtypeStruct((steps, cache_len), f32),
        ),
        in_specs=[pl.BlockSpec(memory_space=pltpu.HBM)] * 2
        + [pl.BlockSpec(memory_space=pltpu.SMEM)],
        scratch_shapes=[
            pltpu.VMEM((steps, heads_dev, key_width), bf16),
            pltpu.VMEM((steps, 1, chosen.shape[2]), jnp.int32),
            pltpu.SemaphoreType.DMA((2,)),
        ],
        compiler_params=pltpu.CompilerParams(vmem_limit_bytes=GRANT),
        name="spread",
    )(
        pltpu.with_memory_space_constraint(queries[0], pltpu.HBM),
        pltpu.with_memory_space_constraint(jnp.swapaxes(chosen, 0, 1), pltpu.HBM),
        position,
    )
    query_all = exchanged(query_all, "seq")
    parts = kernel(
        attend_kernel,
        (shards, steps * CHUNKS + 1, heads_dev, LANES),
        "attend",
        (
            (((steps + 1) // 2, heads, LANES), bf16),
            ((heads, LANES), bf16),
            *(((heads, LATENT), bf16),) * (2 * steps),
        ),
    )(usable, query_all, latent_cache[0].T)
    parts = exchanged(parts, "seq")
    head_out = kernel(merge_kernel, (requests, steps, heads_dev, w_value.shape[2]), "merge")(
        parts, w_value
    )
    head_out = exchanged(head_out, "req")
    features = w_out.shape[1]
    count = requests * steps
    mixed = kernel(
        project_kernel,
        (shards, features // shards // 2, 2 * count),
        "project",
        (((count * heads_dev, LANES), bf16), ((features, 2 * count), f32)),
    )(head_out, w_out.T)
    mixed = exchanged(mixed, "seq")
    return kernel(finish_kernel, (features // shards, count), "finish")(mixed)


def solution(mesh):
    return jax.shard_map(
        body,
        mesh=mesh,
        in_specs=(
            P("req", "seq", None),
            P("req", None, "seq", None),
            P("req", None, None),
            P("req"),
            P("seq", None, None),
            P("seq", "req"),
        ),
        out_specs=P(("req", "seq"), None),
        check_vma=False,
    )
```

```python
import functools
import math

import jax
import jax.numpy as jnp
from jax import lax
from jax.experimental import pallas as pl
from jax.experimental.pallas import tpu as pltpu
from jax.sharding import PartitionSpec as P


LATENT = 512
ROPE = 64
BLOCK = 64
LANES = 128
CHUNKS = LATENT // LANES
STREAMS = ((0, 3),)
GRANT = 12 * 1024 * 1024

score_scale = 1.0 / math.sqrt(192.0)
very_low = -1e30
f32 = jnp.float32
bf16 = jnp.bfloat16


def pieces(value):
    high = value.astype(bf16).astype(f32)
    rest = value - high
    middle = rest.astype(bf16).astype(f32)
    return high, middle, rest - middle


def spread_kernel(query_hbm, *refs):
    *out_refs, query_ref, sem = refs
    copy = pltpu.make_async_copy(query_hbm, query_ref, sem)
    copy.start()
    copy.wait()
    for (begin, end), out_ref in zip(STREAMS, out_refs):
        packed = []
        for t in range(begin, end):
            for c in range(CHUNKS):
                packed.append(query_ref[t, :, c * LANES : (c + 1) * LANES])
        rotary = [query_ref[t, :, LATENT:] for t in range(begin, end)]
        if len(rotary) % 2:
            rotary.append(jnp.zeros_like(rotary[0]))
        for t in range(0, len(rotary), 2):
            packed.append(jnp.concatenate([rotary[t], rotary[t + 1]], axis=1))
        for k, piece in enumerate(packed):
            out_ref[:, k] = jnp.broadcast_to(piece[None], (out_ref.shape[0], *piece.shape))


def mark_kernel(chosen_ref, position_ref, usable_ref):
    steps, cache_len = usable_ref.shape
    blocks = cache_len // BLOCK
    first = lax.axis_index("seq") * cache_len
    column = lax.broadcasted_iota(jnp.int32, (blocks, cache_len), 1)
    mine = column // BLOCK == lax.broadcasted_iota(jnp.int32, (blocks, cache_len), 0)
    mine = mine & (first + column < position_ref[0])
    wanted = chosen_ref.shape[2]
    block = first // BLOCK + lax.broadcasted_iota(jnp.int32, (blocks, wanted), 0)
    for t in range(steps):
        named = jnp.where(chosen_ref[t] == block, 1.0, 0.0)
        named = jnp.max(named, axis=1, keepdims=True)
        usable_ref[t : t + 1, :] = jnp.max(jnp.where(mine, named, 0.0), axis=0, keepdims=True)


def attend_kernel(begin, usable_ref, query_ref, cache_ref, out_ref, rotary_ref, stats_ref, *work):
    shards = query_ref.shape[0]
    steps = len(work) // 2
    heads = rotary_ref.shape[1]
    heads_dev = heads // shards
    spans = [slice(s * heads_dev, (s + 1) * heads_dev) for s in range(shards)]
    for pair in range(rotary_ref.shape[0]):
        for s in range(shards):
            rotary_ref[pair, spans[s], :] = query_ref[s, steps * CHUNKS + pair]
    latent = cache_ref[:LATENT, :]
    rotary_keys = cache_ref[LATENT:, :]
    lane = lax.broadcasted_iota(jnp.int32, (heads, LANES), 1)
    slot = lane % (2 * steps)
    stats = jnp.zeros((heads, LANES), f32)
    for t in range(steps):
        rows_ref, sums_ref = work[2 * t], work[2 * t + 1]
        for c in range(CHUNKS):
            for s in range(shards):
                rows_ref[spans[s], c * LANES : (c + 1) * LANES] = query_ref[s, t * CHUNKS + c]
        rotary = rotary_ref[t // 2, :, (t % 2) * ROPE : (t % 2 + 1) * ROPE]
        scores = jnp.dot(rows_ref[...], latent, preferred_element_type=f32)
        scores = scores + jnp.dot(rotary, rotary_keys, preferred_element_type=f32)
        scores = jnp.where(usable_ref[begin + t : begin + t + 1, :] > 0.0, scores, very_low)
        peak = jnp.max(scores, axis=1, keepdims=True)
        raw = jnp.exp2((scores - peak) * (score_scale * math.log2(math.e)))
        total = jnp.sum(raw, axis=1, keepdims=True)
        sums_ref[...] = lax.dot_general(
            raw.astype(bf16), latent, (((1,), (1,)), ((), ())), preferred_element_type=f32
        ).astype(bf16)
        stats = jnp.where(slot == 2 * t, peak * score_scale, stats)
        stats = jnp.where(slot == 2 * t + 1, total, stats)
        for c in range(CHUNKS):
            for s in range(shards):
                out_ref[s, t * CHUNKS + c] = sums_ref[spans[s], c * LANES : (c + 1) * LANES]
    high, middle, low = pieces(stats)
    stats = jnp.where(lane < 2 * steps, high, jnp.where(lane < 4 * steps, middle, low))
    stats_ref[...] = stats.astype(bf16)
    for s in range(shards):
        out_ref[s, steps * CHUNKS] = stats_ref[spans[s], :]


def merge_kernel(parts_ref, value_ref, out_ref):
    shards, _, heads_dev, _ = parts_ref.shape
    steps = out_ref.shape[0]
    stats = parts_ref[:, steps * CHUNKS].astype(f32)
    latent_out = []
    for t in range(steps):
        peak, total = (
            stats[:, :, k : k + 1]
            + stats[:, :, k + 2 * steps : k + 2 * steps + 1]
            + stats[:, :, k + 4 * steps : k + 4 * steps + 1]
            for k in (2 * t, 2 * t + 1)
        )
        factor = jnp.exp(peak - jnp.max(peak, axis=0, keepdims=True))
        whole = jnp.sum(total * factor, axis=0)
        wide = jnp.broadcast_to(factor, (shards, heads_dev, LANES))
        chunks = []
        for c in range(CHUNKS):
            part = parts_ref[:, t * CHUNKS + c].astype(f32)
            chunks.append(jnp.sum(part * wide, axis=0) / whole)
        latent_out.append(jnp.concatenate(chunks, axis=1))
    latent_out = jnp.concatenate(latent_out, axis=0).astype(bf16)
    row = lax.broadcasted_iota(jnp.int32, (steps * heads_dev, LANES), 0) % heads_dev
    heads = jnp.zeros((steps * heads_dev, LANES), f32)
    for h in range(heads_dev):
        product = jnp.dot(latent_out, value_ref[h], preferred_element_type=f32)
        heads = jnp.where(row == h, product, heads)
    for t in range(steps):
        out_ref[t] = heads[t * heads_dev : (t + 1) * heads_dev, :].astype(bf16)


def merge_last_kernel(parts_ref, value_ref, *refs):
    *earlier_refs, out_ref, heads_ref = refs
    merge_kernel(parts_ref, value_ref, heads_ref)
    t = 0
    for done_ref in (*earlier_refs, heads_ref):
        for k in range(done_ref.shape[0]):
            mine = done_ref[k]
            out_ref[:, t] = jnp.broadcast_to(mine[None], (out_ref.shape[0], *mine.shape))
            t += 1


def pick_kernel(out_ref):
    heads_dev, width, rows = out_ref.shape
    queries = width // 2
    out_row = lax.broadcasted_iota(jnp.int32, (width, rows), 0)
    in_row = lax.broadcasted_iota(jnp.int32, (width, rows), 1)
    source = jnp.where(out_row < queries, out_row, out_row - queries) * heads_dev
    for h in range(heads_dev):
        out_ref[h] = jnp.where(in_row == source + h, 1.0, 0.0).astype(bf16)


def project_kernel(heads_ref, pick_ref, weight_ref, out_ref, flat_ref, wide_ref):
    requests, steps, heads_dev, _ = heads_ref.shape
    queries = requests * steps
    shards, half, width = out_ref.shape
    for q in range(queries):
        flat_ref[q * heads_dev : (q + 1) * heads_dev, :] = heads_ref[q // steps, q % steps]
    every = flat_ref[...]
    mixed = jnp.zeros(wide_ref.shape, f32)
    for h in range(heads_dev):
        of_head = jnp.dot(pick_ref[h], every, preferred_element_type=f32).astype(bf16)
        mixed = mixed + lax.dot_general(
            weight_ref[:, h * LANES : (h + 1) * LANES],
            of_head,
            (((1,), (1,)), ((), ())),
            preferred_element_type=f32,
        )
    wide_ref[...] = mixed
    lane = lax.broadcasted_iota(jnp.int32, (half, width), 1)
    for s in range(shards):
        first = wide_ref[2 * half * s : 2 * half * s + half, :]
        second = wide_ref[2 * half * s + half : 2 * half * (s + 1), :]
        out_ref[s] = jnp.where(lane < queries, first, second).astype(bf16)


def finish_kernel(parts_ref, out_ref):
    _, half, width = parts_ref.shape
    total = jnp.sum(parts_ref[...].astype(f32), axis=0)
    out_ref[:half, :] = total[:, : width // 2].astype(bf16)
    out_ref[half:, :] = total[:, width // 2 :].astype(bf16)


def exchanged(value, axis):
    return lax.all_to_all(value, axis, 0, 0, tiled=True)


def kernel(fn, shape, scratch=(), dtype=bf16):
    return pl.pallas_call(
        fn,
        out_shape=jax.ShapeDtypeStruct(shape, dtype),
        scratch_shapes=[pltpu.VMEM(*s) for s in scratch],
        compiler_params=pltpu.CompilerParams(vmem_limit_bytes=GRANT),
    )


def layer(latent_cache, queries, chosen, position, w_value, w_out):
    cache_len, key_width = latent_cache.shape[1:]
    _, steps, heads_dev, _ = queries.shape
    shards = lax.axis_size("seq")
    requests = lax.axis_size("req")
    heads = shards * heads_dev
    count = requests * steps

    counts = [end - begin for begin, end in STREAMS]
    query_all = pl.pallas_call(
        spread_kernel,
        out_shape=tuple(
            jax.ShapeDtypeStruct((shards, n * CHUNKS + (n + 1) // 2, heads_dev, LANES), bf16)
            for n in counts
        ),
        in_specs=[pl.BlockSpec(memory_space=pltpu.HBM)],
        scratch_shapes=[
            pltpu.VMEM((steps, heads_dev, key_width), bf16),
            pltpu.SemaphoreType.DMA(()),
        ],
        compiler_params=pltpu.CompilerParams(vmem_limit_bytes=GRANT),
        name="spread",
    )(pltpu.with_memory_space_constraint(queries[0], pltpu.HBM))
    query_all = [exchanged(value, "seq") for value in query_all]
    usable = pl.pallas_call(
        mark_kernel,
        out_shape=jax.ShapeDtypeStruct((steps, cache_len), f32),
        in_specs=[
            pl.BlockSpec(memory_space=pltpu.VMEM),
            pl.BlockSpec(memory_space=pltpu.SMEM),
        ],
        compiler_params=pltpu.CompilerParams(vmem_limit_bytes=GRANT),
        name="mark",
    )(jnp.swapaxes(chosen, 0, 1), position)
    pick = kernel(pick_kernel, (heads_dev, 2 * count, count * heads_dev))()
    usable, pick = lax.optimization_barrier((usable, pick))
    parts = []
    for k, n in enumerate(counts):
        part = kernel(
            functools.partial(attend_kernel, STREAMS[k][0]),
            (shards, n * CHUNKS + 1, heads_dev, LANES),
            (
                (((n + 1) // 2, heads, LANES), bf16),
                ((heads, LANES), bf16),
                *(((heads, LATENT), bf16),) * (2 * n),
            ),
        )(usable, query_all[k], latent_cache[0].T)
        parts.append(exchanged(part, "seq"))
    vdim = w_value.shape[2]
    merged = [
        kernel(merge_kernel, (n, heads_dev, vdim))(parts[k], w_value)
        for k, n in enumerate(counts[:-1])
    ]
    head_out = kernel(
        merge_last_kernel,
        (requests, steps, heads_dev, vdim),
        (((counts[-1], heads_dev, vdim), bf16),),
    )(parts[-1], w_value, *merged)
    head_out = exchanged(head_out, "req")
    features = w_out.shape[1]
    mixed = kernel(
        project_kernel,
        (shards, features // shards // 2, 2 * count),
        (((count * heads_dev, LANES), bf16), ((features, 2 * count), f32)),
    )(head_out, pick, w_out.T)
    mixed = exchanged(mixed, "seq")
    return kernel(finish_kernel, (features // shards, count))(mixed)


def solution(mesh):
    return jax.shard_map(
        layer,
        mesh=mesh,
        in_specs=(
            P("req", "seq", None),
            P("req", None, "seq", None),
            P("req", None, None),
            P("req"),
            P("seq", None, None),
            P("seq", "req"),
        ),
        out_specs=P(("req", "seq"), None),
        check_vma=False,
    )
```

```python
import math

import jax
import jax.numpy as jnp
from jax import lax
from jax.experimental import pallas as pl
from jax.experimental.pallas import tpu as pltpu
from jax.sharding import PartitionSpec as P

LATENT = 512
ROPE = 64
BLOCK = 64
LANES = 128
CHUNKS = LATENT // LANES
GRANT = 12 * 1024 * 1024
LAG_NS = 3000

score_scale = 1.0 / math.sqrt(192.0)
very_low = -1e30
f32 = jnp.float32
bf16 = jnp.bfloat16


def pieces(value):
    high = value.astype(bf16).astype(f32)
    rest = value - high
    middle = rest.astype(bf16).astype(f32)
    return high, middle, rest - middle


def spread_kernel(query_hbm, chosen_hbm, position_ref, out_ref, usable_ref, query_ref, chosen_ref, sems):
    copies = [
        pltpu.make_async_copy(source, target, sems.at[k])
        for k, (source, target) in enumerate(
            ((query_hbm, query_ref), (chosen_hbm, chosen_ref))
        )
    ]
    for copy in copies:
        copy.start()
    for copy in copies:
        copy.wait()
    steps, heads_dev, _ = query_ref.shape
    packed = []
    for t in range(steps):
        for c in range(CHUNKS):
            packed.append(query_ref[t, :, c * LANES : (c + 1) * LANES])
    rotary = [query_ref[t, :, LATENT:] for t in range(steps)]
    rotary.append(jnp.zeros_like(rotary[0]))
    for t in range(0, len(rotary), 2):
        packed.append(jnp.concatenate([rotary[t], rotary[t + 1]], axis=1))
    for k, piece in enumerate(packed):
        out_ref[:, k * heads_dev : (k + 1) * heads_dev, :] = jnp.broadcast_to(
            piece[None], (out_ref.shape[0], heads_dev, LANES)
        )
    cache_len = usable_ref.shape[1]
    blocks = cache_len // BLOCK
    first = lax.axis_index("seq") * cache_len
    column = lax.broadcasted_iota(jnp.int32, (blocks, cache_len), 1)
    mine = column // BLOCK == lax.broadcasted_iota(jnp.int32, (blocks, cache_len), 0)
    mine = mine & (first + column < position_ref[0])
    wanted = chosen_ref.shape[2]
    block = first // BLOCK + lax.broadcasted_iota(jnp.int32, (blocks, wanted), 0)
    for t in range(steps):
        named = jnp.where(chosen_ref[t] == block, 1.0, 0.0)
        named = jnp.max(named, axis=1, keepdims=True)
        usable_ref[t : t + 1, :] = jnp.max(jnp.where(mine, named, 0.0), axis=0, keepdims=True)

    @pl.when(lax.axis_index("req") % 2 == 0)
    def _():
        pl.delay(LAG_NS)


def attend_kernel(usable_ref, query_ref, cache_ref, out_ref, rotary_ref, stats_ref, *work):
    shards = query_ref.shape[0]
    steps = usable_ref.shape[0]
    heads = rotary_ref.shape[1]
    heads_dev = heads // shards
    spans = [slice(s * heads_dev, (s + 1) * heads_dev) for s in range(shards)]
    for pair in range(rotary_ref.shape[0]):
        k = (steps * CHUNKS + pair) * heads_dev
        for s in range(shards):
            rotary_ref[pair, spans[s], :] = query_ref[s, k : k + heads_dev, :]
    latent = cache_ref[:LATENT, :]
    rotary_keys = cache_ref[LATENT:, :]
    lane = lax.broadcasted_iota(jnp.int32, (heads, LANES), 1)
    slot = lane % (2 * steps)
    stats = jnp.zeros((heads, LANES), f32)
    for t in range(steps):
        rows_ref, sums_ref = work[2 * t], work[2 * t + 1]
        for c in range(CHUNKS):
            k = (t * CHUNKS + c) * heads_dev
            for s in range(shards):
                rows_ref[spans[s], c * LANES : (c + 1) * LANES] = query_ref[s, k : k + heads_dev, :]
        rotary = rotary_ref[t // 2, :, (t % 2) * ROPE : (t % 2 + 1) * ROPE]
        scores = jnp.dot(rows_ref[...], latent, preferred_element_type=f32)
        scores = scores + jnp.dot(rotary, rotary_keys, preferred_element_type=f32)
        scores = jnp.where(usable_ref[t : t + 1, :] > 0.0, scores, very_low)
        peak = jnp.max(scores, axis=1, keepdims=True)
        raw = jnp.exp2((scores - peak) * (score_scale * math.log2(math.e)))
        total = jnp.sum(raw, axis=1, keepdims=True)
        sums_ref[...] = lax.dot_general(
            raw.astype(bf16), latent, (((1,), (1,)), ((), ())), preferred_element_type=f32
        ).astype(bf16)
        stats = jnp.where(slot == 2 * t, peak * score_scale, stats)
        stats = jnp.where(slot == 2 * t + 1, total, stats)
        for c in range(CHUNKS):
            for s in range(shards):
                out_ref[s, t * CHUNKS + c] = sums_ref[spans[s], c * LANES : (c + 1) * LANES]
    high, middle, low = pieces(stats)
    stats = jnp.where(lane < 2 * steps, high, jnp.where(lane < 4 * steps, middle, low))
    stats_ref[...] = stats.astype(bf16)
    for s in range(shards):
        out_ref[s, steps * CHUNKS] = stats_ref[spans[s], :]


def merge_kernel(parts_ref, value_ref, out_ref):
    shards, _, heads_dev, _ = parts_ref.shape
    requests, steps, _, _ = out_ref.shape
    stats = parts_ref[:, steps * CHUNKS].astype(f32)
    latent_out = []
    for t in range(steps):
        peak, total = (
            stats[:, :, k : k + 1]
            + stats[:, :, k + 2 * steps : k + 2 * steps + 1]
            + stats[:, :, k + 4 * steps : k + 4 * steps + 1]
            for k in (2 * t, 2 * t + 1)
        )
        factor = jnp.exp(peak - jnp.max(peak, axis=0, keepdims=True))
        whole = jnp.sum(total * factor, axis=0)
        wide = jnp.broadcast_to(factor, (shards, heads_dev, LANES))
        chunks = []
        for c in range(CHUNKS):
            part = parts_ref[:, t * CHUNKS + c].astype(f32)
            chunks.append(jnp.sum(part * wide, axis=0) / whole)
        latent_out.append(jnp.concatenate(chunks, axis=1))
    latent_out = jnp.concatenate(latent_out, axis=0).astype(bf16)
    row = lax.broadcasted_iota(jnp.int32, (steps * heads_dev, LANES), 0) % heads_dev
    heads = jnp.zeros((steps * heads_dev, LANES), f32)
    for h in range(heads_dev):
        product = jnp.dot(latent_out, value_ref[h], preferred_element_type=f32)
        heads = jnp.where(row == h, product, heads)
    for t in range(steps):
        mine = heads[t * heads_dev : (t + 1) * heads_dev, :].astype(bf16)
        out_ref[:, t] = jnp.broadcast_to(mine[None], (requests, heads_dev, LANES))


def project_kernel(heads_ref, weight_ref, out_ref, flat_ref, wide_ref):
    requests, steps, heads_dev, _ = heads_ref.shape
    queries = requests * steps
    shards, half, width = out_ref.shape
    for q in range(queries):
        flat_ref[q * heads_dev : (q + 1) * heads_dev, :] = heads_ref[q // steps, q % steps]
    every = flat_ref[...]
    out_row = lax.broadcasted_iota(jnp.int32, (width, queries * heads_dev), 0)
    in_row = lax.broadcasted_iota(jnp.int32, (width, queries * heads_dev), 1)
    source = jnp.where(out_row < queries, out_row, out_row - queries) * heads_dev
    mixed = jnp.zeros(wide_ref.shape, f32)
    for h in range(heads_dev):
        pick = jnp.where(in_row == source + h, 1.0, 0.0).astype(bf16)
        of_head = jnp.dot(pick, every, preferred_element_type=f32).astype(bf16)
        mixed = mixed + lax.dot_general(
            weight_ref[:, h * LANES : (h + 1) * LANES],
            of_head,
            (((1,), (1,)), ((), ())),
            preferred_element_type=f32,
        )
    wide_ref[...] = mixed
    lane = lax.broadcasted_iota(jnp.int32, (half, width), 1)
    for s in range(shards):
        first = wide_ref[2 * half * s : 2 * half * s + half, :]
        second = wide_ref[2 * half * s + half : 2 * half * (s + 1), :]
        out_ref[s] = jnp.where(lane < queries, first, second).astype(bf16)


def finish_kernel(parts_ref, out_ref):
    _, half, width = parts_ref.shape
    total = jnp.sum(parts_ref[...].astype(f32), axis=0)
    out_ref[:half, :] = total[:, : width // 2].astype(bf16)
    out_ref[half:, :] = total[:, width // 2 :].astype(bf16)


def exchanged(value, axis):
    return lax.all_to_all(value, axis, 0, 0, tiled=True)


def kernel(fn, shape, name, scratch=(), dtype=bf16):
    return pl.pallas_call(
        fn,
        out_shape=jax.ShapeDtypeStruct(shape, dtype),
        scratch_shapes=[pltpu.VMEM(*s) for s in scratch],
        compiler_params=pltpu.CompilerParams(vmem_limit_bytes=GRANT),
        name=name,
    )


def body(latent_cache, queries, chosen, position, w_value, w_out):
    cache_len, key_width = latent_cache.shape[1:]
    _, steps, heads_dev, _ = queries.shape
    shards = lax.axis_size("seq")
    requests = lax.axis_size("req")
    heads = shards * heads_dev

    packed_rows = (steps * CHUNKS + (steps + 1) // 2) * heads_dev
    query_all, usable = pl.pallas_call(
        spread_kernel,
        out_shape=(
            jax.ShapeDtypeStruct((shards, packed_rows, LANES), bf16),
            jax.ShapeDtypeStruct((steps, cache_len), f32),
        ),
        in_specs=[pl.BlockSpec(memory_space=pltpu.HBM)] * 2
        + [pl.BlockSpec(memory_space=pltpu.SMEM)],
        scratch_shapes=[
            pltpu.VMEM((steps, heads_dev, key_width), bf16),
            pltpu.VMEM((steps, 1, chosen.shape[2]), jnp.int32),
            pltpu.SemaphoreType.DMA((2,)),
        ],
        compiler_params=pltpu.CompilerParams(vmem_limit_bytes=GRANT),
        name="spread",
    )(
        pltpu.with_memory_space_constraint(queries[0], pltpu.HBM),
        pltpu.with_memory_space_constraint(jnp.swapaxes(chosen, 0, 1), pltpu.HBM),
        position,
    )
    query_all = exchanged(query_all, "seq")
    parts = kernel(
        attend_kernel,
        (shards, steps * CHUNKS + 1, heads_dev, LANES),
        "attend",
        (
            (((steps + 1) // 2, heads, LANES), bf16),
            ((heads, LANES), bf16),
            *(((heads, LATENT), bf16),) * (2 * steps),
        ),
    )(usable, query_all, latent_cache[0].T)
    parts = exchanged(parts, "seq")
    head_out = kernel(merge_kernel, (requests, steps, heads_dev, w_value.shape[2]), "merge")(
        parts, w_value
    )
    head_out = exchanged(head_out, "req")
    features = w_out.shape[1]
    count = requests * steps
    mixed = kernel(
        project_kernel,
        (shards, features // shards // 2, 2 * count),
        "project",
        (((count * heads_dev, LANES), bf16), ((features, 2 * count), f32)),
    )(head_out, w_out.T)
    mixed = exchanged(mixed, "seq")
    return kernel(finish_kernel, (features // shards, count), "finish")(mixed)


def solution(mesh):
    return jax.shard_map(
        body,
        mesh=mesh,
        in_specs=(
            P("req", "seq", None),
            P("req", None, "seq", None),
            P("req", None, None),
            P("req"),
            P("seq", None, None),
            P("seq", "req"),
        ),
        out_specs=P(("req", "seq"), None),
        check_vma=False,
    )
```

```python
import math

import jax
import jax.numpy as jnp
from jax import lax
from jax.experimental import pallas as pl
from jax.experimental.pallas import tpu as pltpu
from jax.sharding import PartitionSpec as P

LATENT = 512
ROPE = 64
BLOCK = 64
LANES = 128
CHUNKS = LATENT // LANES
GRANT = 12 * 1024 * 1024
LAG_NS = 3000

score_scale = 1.0 / math.sqrt(192.0)
very_low = -1e30
f32 = jnp.float32
bf16 = jnp.bfloat16


def pieces(value):
    high = value.astype(bf16).astype(f32)
    rest = value - high
    middle = rest.astype(bf16).astype(f32)
    return high, middle, rest - middle


def spread_kernel(query_hbm, chosen_hbm, position_ref, out_ref, usable_ref, query_ref, chosen_ref, sems):
    copies = [
        pltpu.make_async_copy(source, target, sems.at[k])
        for k, (source, target) in enumerate(
            ((query_hbm, query_ref), (chosen_hbm, chosen_ref))
        )
    ]
    for copy in copies:
        copy.start()
    for copy in copies:
        copy.wait()
    steps, heads_dev, _ = query_ref.shape
    packed = []
    for t in range(steps):
        for c in range(CHUNKS):
            packed.append(query_ref[t, :, c * LANES : (c + 1) * LANES])
    rotary = [query_ref[t, :, LATENT:] for t in range(steps)]
    rotary.append(jnp.zeros_like(rotary[0]))
    for t in range(0, len(rotary), 2):
        packed.append(jnp.concatenate([rotary[t], rotary[t + 1]], axis=1))
    for k, piece in enumerate(packed):
        out_ref[:, k * heads_dev : (k + 1) * heads_dev, :] = jnp.broadcast_to(
            piece[None], (out_ref.shape[0], heads_dev, LANES)
        )
    cache_len = usable_ref.shape[1]
    blocks = cache_len // BLOCK
    first = lax.axis_index("seq") * cache_len
    column = lax.broadcasted_iota(jnp.int32, (blocks, cache_len), 1)
    mine = column // BLOCK == lax.broadcasted_iota(jnp.int32, (blocks, cache_len), 0)
    mine = mine & (first + column < position_ref[0])
    wanted = chosen_ref.shape[2]
    block = first // BLOCK + lax.broadcasted_iota(jnp.int32, (blocks, wanted), 0)
    for t in range(steps):
        named = jnp.where(chosen_ref[t] == block, 1.0, 0.0)
        named = jnp.max(named, axis=1, keepdims=True)
        usable_ref[t : t + 1, :] = jnp.max(jnp.where(mine, named, 0.0), axis=0, keepdims=True)

    @pl.when(lax.axis_index("req") % 2 == 0)
    def _():
        pl.delay(LAG_NS)


def attend_kernel(usable_ref, query_ref, cache_ref, out_ref, rows_ref, rotary_ref, sums_ref, stats_ref):
    shards = query_ref.shape[0]
    steps = usable_ref.shape[0]
    heads = rotary_ref.shape[1]
    heads_dev = heads // shards
    for pair in range(rotary_ref.shape[0]):
        k = (steps * CHUNKS + pair) * heads_dev
        for s in range(shards):
            rotary_ref[pair, s * heads_dev : (s + 1) * heads_dev, :] = query_ref[s, k : k + heads_dev, :]
    for t in range(steps):
        for c in range(CHUNKS):
            k = (t * CHUNKS + c) * heads_dev
            for s in range(shards):
                row = t * heads + s * heads_dev
                rows_ref[row : row + heads_dev, c * LANES : (c + 1) * LANES] = query_ref[
                    s, k : k + heads_dev, :
                ]
    rotary = jnp.concatenate(
        [rotary_ref[t // 2, :, (t % 2) * ROPE : (t % 2 + 1) * ROPE] for t in range(steps)], axis=0
    )
    every = jnp.dot(rows_ref[...], cache_ref[:LATENT, :], preferred_element_type=f32)
    every = every + jnp.dot(rotary, cache_ref[LATENT:, :], preferred_element_type=f32)
    lane = lax.broadcasted_iota(jnp.int32, (heads, LANES), 1)
    slot = lane % (2 * steps)
    stats = jnp.zeros((heads, LANES), f32)
    weights = []
    for t in range(steps):
        scores = every[t * heads : (t + 1) * heads]
        scores = jnp.where(usable_ref[t : t + 1, :] > 0.0, scores, very_low)
        peak = jnp.max(scores, axis=1, keepdims=True)
        raw = jnp.exp2((scores - peak) * (score_scale * math.log2(math.e)))
        total = jnp.sum(raw, axis=1, keepdims=True)
        weights.append(raw.astype(bf16))
        stats = jnp.where(slot == 2 * t, peak * score_scale, stats)
        stats = jnp.where(slot == 2 * t + 1, total, stats)
    sums_ref[...] = lax.dot_general(
        jnp.concatenate(weights, axis=0),
        cache_ref[:LATENT, :],
        (((1,), (1,)), ((), ())),
        preferred_element_type=f32,
    ).astype(bf16)
    high, middle, low = pieces(stats)
    stats = jnp.where(lane < 2 * steps, high, jnp.where(lane < 4 * steps, middle, low))
    stats_ref[...] = stats.astype(bf16)
    for s in range(shards):
        for t in range(steps):
            row = t * heads + s * heads_dev
            for c in range(CHUNKS):
                out_ref[s, t * CHUNKS + c] = sums_ref[
                    row : row + heads_dev, c * LANES : (c + 1) * LANES
                ]
        out_ref[s, steps * CHUNKS] = stats_ref[s * heads_dev : (s + 1) * heads_dev, :]


def merge_kernel(parts_ref, value_ref, out_ref):
    shards, _, heads_dev, _ = parts_ref.shape
    requests, steps, _, _ = out_ref.shape
    stats = parts_ref[:, steps * CHUNKS].astype(f32)
    latent_out = []
    for t in range(steps):
        peak, total = (
            stats[:, :, k : k + 1]
            + stats[:, :, k + 2 * steps : k + 2 * steps + 1]
            + stats[:, :, k + 4 * steps : k + 4 * steps + 1]
            for k in (2 * t, 2 * t + 1)
        )
        factor = jnp.exp(peak - jnp.max(peak, axis=0, keepdims=True))
        whole = jnp.sum(total * factor, axis=0)
        wide = jnp.broadcast_to(factor, (shards, heads_dev, LANES))
        chunks = []
        for c in range(CHUNKS):
            part = parts_ref[:, t * CHUNKS + c].astype(f32)
            chunks.append(jnp.sum(part * wide, axis=0) / whole)
        latent_out.append(jnp.concatenate(chunks, axis=1))
    latent_out = jnp.concatenate(latent_out, axis=0).astype(bf16)
    row = lax.broadcasted_iota(jnp.int32, (steps * heads_dev, LANES), 0) % heads_dev
    heads = jnp.zeros((steps * heads_dev, LANES), f32)
    for h in range(heads_dev):
        product = jnp.dot(latent_out, value_ref[h], preferred_element_type=f32)
        heads = jnp.where(row == h, product, heads)
    for t in range(steps):
        mine = heads[t * heads_dev : (t + 1) * heads_dev, :].astype(bf16)
        out_ref[:, t] = jnp.broadcast_to(mine[None], (requests, heads_dev, LANES))


def project_kernel(heads_ref, weight_ref, out_ref, flat_ref, wide_ref):
    requests, steps, heads_dev, _ = heads_ref.shape
    queries = requests * steps
    shards, half, width = out_ref.shape
    for q in range(queries):
        flat_ref[q * heads_dev : (q + 1) * heads_dev, :] = heads_ref[q // steps, q % steps]
    every = flat_ref[...]
    out_row = lax.broadcasted_iota(jnp.int32, (width, queries * heads_dev), 0)
    in_row = lax.broadcasted_iota(jnp.int32, (width, queries * heads_dev), 1)
    source = jnp.where(out_row < queries, out_row, out_row - queries) * heads_dev
    of_heads = []
    for h in range(heads_dev):
        pick = jnp.where(in_row == source + h, 1.0, 0.0).astype(bf16)
        of_heads.append(jnp.dot(pick, every, preferred_element_type=f32).astype(bf16))
    wide_ref[...] = lax.dot_general(
        weight_ref[...],
        jnp.concatenate(of_heads, axis=1),
        (((1,), (1,)), ((), ())),
        preferred_element_type=f32,
    )
    lane = lax.broadcasted_iota(jnp.int32, (half, width), 1)
    for s in range(shards):
        first = wide_ref[2 * half * s : 2 * half * s + half, :]
        second = wide_ref[2 * half * s + half : 2 * half * (s + 1), :]
        out_ref[s] = jnp.where(lane < queries, first, second).astype(bf16)


def finish_kernel(parts_ref, out_ref):
    _, half, width = parts_ref.shape
    total = jnp.sum(parts_ref[...].astype(f32), axis=0)
    out_ref[:half, :] = total[:, : width // 2].astype(bf16)
    out_ref[half:, :] = total[:, width // 2 :].astype(bf16)


def exchanged(value, axis):
    return lax.all_to_all(value, axis, 0, 0, tiled=True)


def kernel(fn, shape, name, scratch=(), dtype=bf16):
    return pl.pallas_call(
        fn,
        out_shape=jax.ShapeDtypeStruct(shape, dtype),
        scratch_shapes=[pltpu.VMEM(*s) for s in scratch],
        compiler_params=pltpu.CompilerParams(vmem_limit_bytes=GRANT),
        name=name,
    )


def body(latent_cache, queries, chosen, position, w_value, w_out):
    cache_len, key_width = latent_cache.shape[1:]
    _, steps, heads_dev, _ = queries.shape
    shards = lax.axis_size("seq")
    requests = lax.axis_size("req")
    heads = shards * heads_dev

    packed_rows = (steps * CHUNKS + (steps + 1) // 2) * heads_dev
    query_all, usable = pl.pallas_call(
        spread_kernel,
        out_shape=(
            jax.ShapeDtypeStruct((shards, packed_rows, LANES), bf16),
            jax.ShapeDtypeStruct((steps, cache_len), f32),
        ),
        in_specs=[pl.BlockSpec(memory_space=pltpu.HBM)] * 2
        + [pl.BlockSpec(memory_space=pltpu.SMEM)],
        scratch_shapes=[
            pltpu.VMEM((steps, heads_dev, key_width), bf16),
            pltpu.VMEM((steps, 1, chosen.shape[2]), jnp.int32),
            pltpu.SemaphoreType.DMA((2,)),
        ],
        compiler_params=pltpu.CompilerParams(vmem_limit_bytes=GRANT),
        name="spread",
    )(
        pltpu.with_memory_space_constraint(queries[0], pltpu.HBM),
        pltpu.with_memory_space_constraint(jnp.swapaxes(chosen, 0, 1), pltpu.HBM),
        position,
    )
    query_all = exchanged(query_all, "seq")
    parts = kernel(
        attend_kernel,
        (shards, steps * CHUNKS + 1, heads_dev, LANES),
        "attend",
        (
            ((steps * heads, LATENT), bf16),
            (((steps + 1) // 2, heads, LANES), bf16),
            ((steps * heads, LATENT), bf16),
            ((heads, LANES), bf16),
        ),
    )(usable, query_all, latent_cache[0].T)
    parts = exchanged(parts, "seq")
    head_out = kernel(merge_kernel, (requests, steps, heads_dev, w_value.shape[2]), "merge")(
        parts, w_value
    )
    head_out = exchanged(head_out, "req")
    features = w_out.shape[1]
    count = requests * steps
    mixed = kernel(
        project_kernel,
        (shards, features // shards // 2, 2 * count),
        "project",
        (((count * heads_dev, LANES), bf16), ((features, 2 * count), f32)),
    )(head_out, w_out.T)
    mixed = exchanged(mixed, "seq")
    return kernel(finish_kernel, (features // shards, count), "finish")(mixed)


def solution(mesh):
    return jax.shard_map(
        body,
        mesh=mesh,
        in_specs=(
            P("req", "seq", None),
            P("req", None, "seq", None),
            P("req", None, None),
            P("req"),
            P("seq", None, None),
            P("seq", "req"),
        ),
        out_specs=P(("req", "seq"), None),
        check_vma=False,
    )
```

```python
import math

import jax
import jax.numpy as jnp
from jax import lax
from jax.experimental import pallas as pl
from jax.experimental.pallas import tpu as pltpu
from jax.sharding import PartitionSpec as P

LATENT = 512
ROPE = 64
BLOCK = 64
LANES = 128
CHUNKS = LATENT // LANES
GRANT = 12 * 1024 * 1024
LAG_NS = 3000

score_scale = 1.0 / math.sqrt(192.0)
very_low = -1e30
f32 = jnp.float32
bf16 = jnp.bfloat16


def pieces(value):
    high = value.astype(bf16).astype(f32)
    rest = value - high
    middle = rest.astype(bf16).astype(f32)
    return high, middle, rest - middle


def spread_kernel(query_hbm, chosen_hbm, position_ref, out_ref, usable_ref, query_ref, chosen_ref, sems):
    copies = [
        pltpu.make_async_copy(source, target, sems.at[k])
        for k, (source, target) in enumerate(
            ((query_hbm, query_ref), (chosen_hbm, chosen_ref))
        )
    ]
    for copy in copies:
        copy.start()
    for copy in copies:
        copy.wait()
    steps, heads_dev, _ = query_ref.shape
    packed = []
    for t in range(steps):
        for c in range(CHUNKS):
            packed.append(query_ref[t, :, c * LANES : (c + 1) * LANES])
    rotary = [query_ref[t, :, LATENT:] for t in range(steps)]
    rotary.append(jnp.zeros_like(rotary[0]))
    for t in range(0, len(rotary), 2):
        packed.append(jnp.concatenate([rotary[t], rotary[t + 1]], axis=1))
    for k in range(0, len(packed), 2):
        tile = jnp.concatenate(packed[k : k + 2], axis=0)
        out_ref[:, k * heads_dev : (k + 2) * heads_dev, :] = jnp.broadcast_to(
            tile[None], (out_ref.shape[0], *tile.shape)
        )
    cache_len = usable_ref.shape[1]
    blocks = cache_len // BLOCK
    first = lax.axis_index("seq") * cache_len
    column = lax.broadcasted_iota(jnp.int32, (blocks, cache_len), 1)
    mine = column // BLOCK == lax.broadcasted_iota(jnp.int32, (blocks, cache_len), 0)
    mine = mine & (first + column < position_ref[0])
    wanted = chosen_ref.shape[2]
    block = first // BLOCK + lax.broadcasted_iota(jnp.int32, (blocks, wanted), 0)
    for t in range(steps):
        named = jnp.where(chosen_ref[t] == block, 1.0, 0.0)
        named = jnp.max(named, axis=1, keepdims=True)
        usable_ref[t : t + 1, :] = jnp.max(jnp.where(mine, named, 0.0), axis=0, keepdims=True)

    @pl.when(lax.axis_index("req") % 2 == 0)
    def _():
        pl.delay(LAG_NS)


def attend_kernel(usable_ref, query_ref, cache_ref, out_ref, rows_ref, rotary_ref, sums_ref, stats_ref):
    shards = query_ref.shape[0]
    steps = usable_ref.shape[0]
    heads = rotary_ref.shape[1]
    heads_dev = heads // shards
    for pair in range(rotary_ref.shape[0]):
        k = (steps * CHUNKS + pair) * heads_dev
        for s in range(shards):
            rotary_ref[pair, s * heads_dev : (s + 1) * heads_dev, :] = query_ref[s, k : k + heads_dev, :]
    for t in range(steps):
        for c in range(CHUNKS):
            k = (t * CHUNKS + c) * heads_dev
            for s in range(shards):
                row = t * heads + s * heads_dev
                rows_ref[row : row + heads_dev, c * LANES : (c + 1) * LANES] = query_ref[
                    s, k : k + heads_dev, :
                ]
    rotary = jnp.concatenate(
        [rotary_ref[t // 2, :, (t % 2) * ROPE : (t % 2 + 1) * ROPE] for t in range(steps)], axis=0
    )
    every = jnp.dot(rows_ref[...], cache_ref[:LATENT, :], preferred_element_type=f32)
    every = every + jnp.dot(rotary, cache_ref[LATENT:, :], preferred_element_type=f32)
    lane = lax.broadcasted_iota(jnp.int32, (heads, LANES), 1)
    slot = lane % (2 * steps)
    stats = jnp.zeros((heads, LANES), f32)
    weights = []
    for t in range(steps):
        scores = every[t * heads : (t + 1) * heads]
        scores = jnp.where(usable_ref[t : t + 1, :] > 0.0, scores, very_low)
        peak = jnp.max(scores, axis=1, keepdims=True)
        raw = jnp.exp2((scores - peak) * (score_scale * math.log2(math.e)))
        total = jnp.sum(raw, axis=1, keepdims=True)
        weights.append(raw.astype(bf16))
        stats = jnp.where(slot == 2 * t, peak * score_scale, stats)
        stats = jnp.where(slot == 2 * t + 1, total, stats)
    sums_ref[...] = lax.dot_general(
        jnp.concatenate(weights, axis=0),
        cache_ref[:LATENT, :],
        (((1,), (1,)), ((), ())),
        preferred_element_type=f32,
    ).astype(bf16)
    high, middle, low = pieces(stats)
    stats = jnp.where(lane < 2 * steps, high, jnp.where(lane < 4 * steps, middle, low))
    stats_ref[...] = stats.astype(bf16)
    for s in range(shards):
        for t in range(steps):
            row = t * heads + s * heads_dev
            for c in range(CHUNKS):
                out_ref[s, t * CHUNKS + c] = sums_ref[
                    row : row + heads_dev, c * LANES : (c + 1) * LANES
                ]
        out_ref[s, steps * CHUNKS] = stats_ref[s * heads_dev : (s + 1) * heads_dev, :]


def merge_kernel(parts_ref, value_ref, out_ref):
    shards, _, heads_dev, _ = parts_ref.shape
    requests, steps, _, _ = out_ref.shape
    stats = parts_ref[:, steps * CHUNKS].astype(f32)

    def shifted(value, by):
        return pltpu.roll(value, LANES - by, 2)

    stats = stats + shifted(stats, 2 * steps) + shifted(stats, 4 * steps)
    factors = jnp.exp(stats - jnp.max(stats, axis=0, keepdims=True))
    wholes = jnp.sum(shifted(stats, 1) * factors, axis=0)
    latent_out = []
    for t in range(steps):
        whole = wholes[:, 2 * t : 2 * t + 1]
        wide = jnp.broadcast_to(factors[:, :, 2 * t : 2 * t + 1], (shards, heads_dev, LANES))
        chunks = []
        for c in range(CHUNKS):
            part = parts_ref[:, t * CHUNKS + c].astype(f32)
            chunks.append(jnp.sum(part * wide, axis=0) / whole)
        latent_out.append(jnp.concatenate(chunks, axis=1))
    latent_out = jnp.concatenate(latent_out, axis=0).astype(bf16)
    row = lax.broadcasted_iota(jnp.int32, (steps * heads_dev, LANES), 0) % heads_dev
    every = jnp.dot(
        latent_out,
        jnp.concatenate([value_ref[h] for h in range(heads_dev)], axis=1),
        preferred_element_type=f32,
    )
    heads = every[:, :LANES]
    for h in range(1, heads_dev):
        heads = jnp.where(row == h, every[:, h * LANES : (h + 1) * LANES], heads)
    for t in range(steps):
        mine = heads[t * heads_dev : (t + 1) * heads_dev, :].astype(bf16)
        out_ref[:, t] = jnp.broadcast_to(mine[None], (requests, heads_dev, LANES))


def project_kernel(heads_ref, weight_ref, out_ref, flat_ref, wide_ref):
    requests, steps, heads_dev, _ = heads_ref.shape
    queries = requests * steps
    shards, half, width = out_ref.shape
    for q in range(queries):
        flat_ref[q * heads_dev : (q + 1) * heads_dev, :] = heads_ref[q // steps, q % steps]
    every = flat_ref[...]
    out_row = lax.broadcasted_iota(jnp.int32, (width, queries * heads_dev), 0)
    in_row = lax.broadcasted_iota(jnp.int32, (width, queries * heads_dev), 1)
    source = jnp.where(out_row < queries, out_row, out_row - queries) * heads_dev
    of_heads = []
    for h in range(heads_dev):
        pick = jnp.where(in_row == source + h, 1.0, 0.0).astype(bf16)
        of_heads.append(jnp.dot(pick, every, preferred_element_type=f32).astype(bf16))
    wide_ref[...] = lax.dot_general(
        weight_ref[...],
        jnp.concatenate(of_heads, axis=1),
        (((1,), (1,)), ((), ())),
        preferred_element_type=f32,
    )
    lane = lax.broadcasted_iota(jnp.int32, (half, width), 1)
    for s in range(shards):
        first = wide_ref[2 * half * s : 2 * half * s + half, :]
        second = wide_ref[2 * half * s + half : 2 * half * (s + 1), :]
        out_ref[s] = jnp.where(lane < queries, first, second).astype(bf16)


def finish_kernel(parts_ref, out_ref):
    _, half, width = parts_ref.shape
    total = jnp.sum(parts_ref[...].astype(f32), axis=0)
    out_ref[:half, :] = total[:, : width // 2].astype(bf16)
    out_ref[half:, :] = total[:, width // 2 :].astype(bf16)


def exchanged(value, axis):
    return lax.all_to_all(value, axis, 0, 0, tiled=True)


def kernel(fn, shape, name, scratch=(), dtype=bf16):
    return pl.pallas_call(
        fn,
        out_shape=jax.ShapeDtypeStruct(shape, dtype),
        scratch_shapes=[pltpu.VMEM(*s) for s in scratch],
        compiler_params=pltpu.CompilerParams(vmem_limit_bytes=GRANT),
        name=name,
    )


def body(latent_cache, queries, chosen, position, w_value, w_out):
    cache_len, key_width = latent_cache.shape[1:]
    _, steps, heads_dev, _ = queries.shape
    shards = lax.axis_size("seq")
    requests = lax.axis_size("req")
    heads = shards * heads_dev

    packed_rows = (steps * CHUNKS + (steps + 1) // 2) * heads_dev
    query_all, usable = pl.pallas_call(
        spread_kernel,
        out_shape=(
            jax.ShapeDtypeStruct((shards, packed_rows, LANES), bf16),
            jax.ShapeDtypeStruct((steps, cache_len), f32),
        ),
        in_specs=[pl.BlockSpec(memory_space=pltpu.HBM)] * 2
        + [pl.BlockSpec(memory_space=pltpu.SMEM)],
        scratch_shapes=[
            pltpu.VMEM((steps, heads_dev, key_width), bf16),
            pltpu.VMEM((steps, 1, chosen.shape[2]), jnp.int32),
            pltpu.SemaphoreType.DMA((2,)),
        ],
        compiler_params=pltpu.CompilerParams(vmem_limit_bytes=GRANT),
        name="spread",
    )(
        pltpu.with_memory_space_constraint(queries[0], pltpu.HBM),
        pltpu.with_memory_space_constraint(jnp.swapaxes(chosen, 0, 1), pltpu.HBM),
        position,
    )
    query_all = exchanged(query_all, "seq")
    parts = kernel(
        attend_kernel,
        (shards, steps * CHUNKS + 1, heads_dev, LANES),
        "attend",
        (
            ((steps * heads, LATENT), bf16),
            (((steps + 1) // 2, heads, LANES), bf16),
            ((steps * heads, LATENT), bf16),
            ((heads, LANES), bf16),
        ),
    )(usable, query_all, latent_cache[0].T)
    parts = exchanged(parts, "seq")
    head_out = kernel(merge_kernel, (requests, steps, heads_dev, w_value.shape[2]), "merge")(
        parts, w_value
    )
    head_out = exchanged(head_out, "req")
    features = w_out.shape[1]
    count = requests * steps
    mixed = kernel(
        project_kernel,
        (shards, features // shards // 2, 2 * count),
        "project",
        (((count * heads_dev, LANES), bf16), ((features, 2 * count), f32)),
    )(head_out, w_out.T)
    mixed = exchanged(mixed, "seq")
    return kernel(finish_kernel, (features // shards, count), "finish")(mixed)


def solution(mesh):
    return jax.shard_map(
        body,
        mesh=mesh,
        in_specs=(
            P("req", "seq", None),
            P("req", None, "seq", None),
            P("req", None, None),
            P("req"),
            P("seq", None, None),
            P("seq", "req"),
        ),
        out_specs=P(("req", "seq"), None),
        check_vma=False,
    )
```

```python
import math

import jax
import jax.numpy as jnp
from jax import lax
from jax.experimental import pallas as pl
from jax.experimental.pallas import tpu as pltpu
from jax.sharding import PartitionSpec as P

LATENT = 512
ROPE = 64
BLOCK = 64
LANES = 128
CHUNKS = LATENT // LANES
GRANT = 12 * 1024 * 1024
LAG_NS = 2000

score_scale = 1.0 / math.sqrt(192.0)
very_low = -1e30
f32 = jnp.float32
bf16 = jnp.bfloat16


def pieces(value):
    high = value.astype(bf16).astype(f32)
    rest = value - high
    middle = rest.astype(bf16).astype(f32)
    return high, middle, rest - middle


def spread_kernel(query_hbm, chosen_hbm, position_ref, out_ref, usable_ref, query_ref, chosen_ref, sems):
    copies = [
        pltpu.make_async_copy(source, target, sems.at[k])
        for k, (source, target) in enumerate(
            ((query_hbm, query_ref), (chosen_hbm, chosen_ref))
        )
    ]
    for copy in copies:
        copy.start()
    for copy in copies:
        copy.wait()
    steps, heads_dev, _ = query_ref.shape
    packed = []
    for t in range(steps):
        for c in range(CHUNKS):
            packed.append(query_ref[t, :, c * LANES : (c + 1) * LANES])
    rotary = [query_ref[t, :, LATENT:] for t in range(steps)]
    rotary.append(jnp.zeros_like(rotary[0]))
    for t in range(0, len(rotary), 2):
        packed.append(jnp.concatenate([rotary[t], rotary[t + 1]], axis=1))
    for k in range(0, len(packed), 2):
        tile = jnp.concatenate(packed[k : k + 2], axis=0)
        out_ref[:, k * heads_dev : (k + 2) * heads_dev, :] = jnp.broadcast_to(
            tile[None], (out_ref.shape[0], *tile.shape)
        )
    cache_len = usable_ref.shape[1]
    blocks = cache_len // BLOCK
    first = lax.axis_index("seq") * cache_len
    column = lax.broadcasted_iota(jnp.int32, (blocks, cache_len), 1)
    mine = column // BLOCK == lax.broadcasted_iota(jnp.int32, (blocks, cache_len), 0)
    mine = mine & (first + column < position_ref[0])
    wanted = chosen_ref.shape[2]
    block = first // BLOCK + lax.broadcasted_iota(jnp.int32, (blocks, wanted), 0)
    for t in range(steps):
        named = jnp.where(chosen_ref[t] == block, 1.0, 0.0)
        named = jnp.max(named, axis=1, keepdims=True)
        usable_ref[t : t + 1, :] = jnp.max(jnp.where(mine, named, 0.0), axis=0, keepdims=True)

    @pl.when(lax.axis_index("req") % 2 == 0)
    def _():
        pl.delay(LAG_NS)


def attend_kernel(usable_ref, query_ref, cache_ref, out_ref, rows_ref, rotary_ref, sums_ref, stats_ref):
    shards = query_ref.shape[0]
    steps = usable_ref.shape[0]
    heads = rotary_ref.shape[1]
    heads_dev = heads // shards
    for pair in range(rotary_ref.shape[0]):
        k = (steps * CHUNKS + pair) * heads_dev
        for s in range(shards):
            rotary_ref[pair, s * heads_dev : (s + 1) * heads_dev, :] = query_ref[s, k : k + heads_dev, :]
    for t in range(steps):
        for c in range(CHUNKS):
            k = (t * CHUNKS + c) * heads_dev
            for s in range(shards):
                row = t * heads + s * heads_dev
                rows_ref[row : row + heads_dev, c * LANES : (c + 1) * LANES] = query_ref[
                    s, k : k + heads_dev, :
                ]
    rotary = jnp.concatenate(
        [rotary_ref[t // 2, :, (t % 2) * ROPE : (t % 2 + 1) * ROPE] for t in range(steps)], axis=0
    )
    every = jnp.dot(rows_ref[...], cache_ref[:LATENT, :], preferred_element_type=f32)
    every = every + jnp.dot(rotary, cache_ref[LATENT:, :], preferred_element_type=f32)
    lane = lax.broadcasted_iota(jnp.int32, (heads, LANES), 1)
    slot = lane % (2 * steps)
    stats = jnp.zeros((heads, LANES), f32)
    weights = []
    for t in range(steps):
        scores = every[t * heads : (t + 1) * heads]
        scores = jnp.where(usable_ref[t : t + 1, :] > 0.0, scores, very_low)
        peak = jnp.max(scores, axis=1, keepdims=True)
        raw = jnp.exp2((scores - peak) * (score_scale * math.log2(math.e)))
        total = jnp.sum(raw, axis=1, keepdims=True)
        weights.append(raw.astype(bf16))
        stats = jnp.where(slot == 2 * t, peak * score_scale, stats)
        stats = jnp.where(slot == 2 * t + 1, total, stats)
    sums_ref[...] = lax.dot_general(
        jnp.concatenate(weights, axis=0),
        cache_ref[:LATENT, :],
        (((1,), (1,)), ((), ())),
        preferred_element_type=f32,
    ).astype(bf16)
    high, middle, low = pieces(stats)
    stats = jnp.where(lane < 2 * steps, high, jnp.where(lane < 4 * steps, middle, low))
    stats_ref[...] = stats.astype(bf16)
    for s in range(shards):
        for t in range(steps):
            row = t * heads + s * heads_dev
            for c in range(CHUNKS):
                out_ref[s, t * CHUNKS + c] = sums_ref[
                    row : row + heads_dev, c * LANES : (c + 1) * LANES
                ]
        out_ref[s, steps * CHUNKS] = stats_ref[s * heads_dev : (s + 1) * heads_dev, :]


def merge_kernel(parts_ref, value_ref, out_ref):
    shards, _, heads_dev, _ = parts_ref.shape
    requests, steps, _, _ = out_ref.shape
    stats = parts_ref[:, steps * CHUNKS].astype(f32)

    def shifted(value, by):
        return pltpu.roll(value, LANES - by, 2)

    stats = stats + shifted(stats, 2 * steps) + shifted(stats, 4 * steps)
    factors = jnp.exp(stats - jnp.max(stats, axis=0, keepdims=True))
    wholes = jnp.sum(shifted(stats, 1) * factors, axis=0)
    latent_out = []
    for t in range(steps):
        whole = wholes[:, 2 * t : 2 * t + 1]
        wide = jnp.broadcast_to(factors[:, :, 2 * t : 2 * t + 1], (shards, heads_dev, LANES))
        chunks = []
        for c in range(CHUNKS):
            part = parts_ref[:, t * CHUNKS + c].astype(f32)
            chunks.append(jnp.sum(part * wide, axis=0) / whole)
        latent_out.append(jnp.concatenate(chunks, axis=1))
    latent_out = jnp.concatenate(latent_out, axis=0).astype(bf16)
    row = lax.broadcasted_iota(jnp.int32, (steps * heads_dev, LANES), 0) % heads_dev
    every = jnp.dot(
        latent_out,
        jnp.concatenate([value_ref[h] for h in range(heads_dev)], axis=1),
        preferred_element_type=f32,
    )
    heads = every[:, :LANES]
    for h in range(1, heads_dev):
        heads = jnp.where(row == h, every[:, h * LANES : (h + 1) * LANES], heads)
    for t in range(steps):
        mine = heads[t * heads_dev : (t + 1) * heads_dev, :].astype(bf16)
        out_ref[:, t] = jnp.broadcast_to(mine[None], (requests, heads_dev, LANES))


def project_kernel(heads_ref, weight_ref, out_ref, flat_ref, wide_ref):
    requests, steps, heads_dev, _ = heads_ref.shape
    queries = requests * steps
    shards, half, width = out_ref.shape
    for q in range(queries):
        flat_ref[q * heads_dev : (q + 1) * heads_dev, :] = heads_ref[q // steps, q % steps]
    every = flat_ref[...]
    out_row = lax.broadcasted_iota(jnp.int32, (width, queries * heads_dev), 0)
    in_row = lax.broadcasted_iota(jnp.int32, (width, queries * heads_dev), 1)
    source = jnp.where(out_row < queries, out_row, out_row - queries) * heads_dev
    of_heads = []
    for h in range(heads_dev):
        pick = jnp.where(in_row == source + h, 1.0, 0.0).astype(bf16)
        of_heads.append(jnp.dot(pick, every, preferred_element_type=f32).astype(bf16))
    wide_ref[...] = lax.dot_general(
        weight_ref[...],
        jnp.concatenate(of_heads, axis=1),
        (((1,), (1,)), ((), ())),
        preferred_element_type=f32,
    )
    lane = lax.broadcasted_iota(jnp.int32, (half, width), 1)
    for s in range(shards):
        first = wide_ref[2 * half * s : 2 * half * s + half, :]
        second = wide_ref[2 * half * s + half : 2 * half * (s + 1), :]
        out_ref[s] = jnp.where(lane < queries, first, second).astype(bf16)


def finish_kernel(parts_ref, out_ref):
    _, half, width = parts_ref.shape
    total = jnp.sum(parts_ref[...].astype(f32), axis=0)
    out_ref[:half, :] = total[:, : width // 2].astype(bf16)
    out_ref[half:, :] = total[:, width // 2 :].astype(bf16)


def exchanged(value, axis):
    return lax.all_to_all(value, axis, 0, 0, tiled=True)


def kernel(fn, shape, name, scratch=(), dtype=bf16):
    return pl.pallas_call(
        fn,
        out_shape=jax.ShapeDtypeStruct(shape, dtype),
        scratch_shapes=[pltpu.VMEM(*s) for s in scratch],
        compiler_params=pltpu.CompilerParams(vmem_limit_bytes=GRANT),
        name=name,
    )


def body(latent_cache, queries, chosen, position, w_value, w_out):
    cache_len, key_width = latent_cache.shape[1:]
    _, steps, heads_dev, _ = queries.shape
    shards = lax.axis_size("seq")
    requests = lax.axis_size("req")
    heads = shards * heads_dev

    packed_rows = (steps * CHUNKS + (steps + 1) // 2) * heads_dev
    query_all, usable = pl.pallas_call(
        spread_kernel,
        out_shape=(
            jax.ShapeDtypeStruct((shards, packed_rows, LANES), bf16),
            jax.ShapeDtypeStruct((steps, cache_len), f32),
        ),
        in_specs=[pl.BlockSpec(memory_space=pltpu.HBM)] * 2
        + [pl.BlockSpec(memory_space=pltpu.SMEM)],
        scratch_shapes=[
            pltpu.VMEM((steps, heads_dev, key_width), bf16),
            pltpu.VMEM((steps, 1, chosen.shape[2]), jnp.int32),
            pltpu.SemaphoreType.DMA((2,)),
        ],
        compiler_params=pltpu.CompilerParams(vmem_limit_bytes=GRANT),
        name="spread",
    )(
        pltpu.with_memory_space_constraint(queries[0], pltpu.HBM),
        pltpu.with_memory_space_constraint(jnp.swapaxes(chosen, 0, 1), pltpu.HBM),
        position,
    )
    query_all = exchanged(query_all, "seq")
    parts = kernel(
        attend_kernel,
        (shards, steps * CHUNKS + 1, heads_dev, LANES),
        "attend",
        (
            ((steps * heads, LATENT), bf16),
            (((steps + 1) // 2, heads, LANES), bf16),
            ((steps * heads, LATENT), bf16),
            ((heads, LANES), bf16),
        ),
    )(usable, query_all, latent_cache[0].T)
    parts = exchanged(parts, "seq")
    head_out = kernel(merge_kernel, (requests, steps, heads_dev, w_value.shape[2]), "merge")(
        parts, w_value
    )
    head_out = exchanged(head_out, "req")
    features = w_out.shape[1]
    count = requests * steps
    mixed = kernel(
        project_kernel,
        (shards, features // shards // 2, 2 * count),
        "project",
        (((count * heads_dev, LANES), bf16), ((features, 2 * count), f32)),
    )(head_out, w_out.T)
    mixed = exchanged(mixed, "seq")
    return kernel(finish_kernel, (features // shards, count), "finish")(mixed)


def solution(mesh):
    return jax.shard_map(
        body,
        mesh=mesh,
        in_specs=(
            P("req", "seq", None),
            P("req", None, "seq", None),
            P("req", None, None),
            P("req"),
            P("seq", None, None),
            P("seq", "req"),
        ),
        out_specs=P(("req", "seq"), None),
        check_vma=False,
    )
```

```python
import math

import jax
import jax.numpy as jnp
from jax import lax
from jax.experimental import pallas as pl
from jax.experimental.pallas import tpu as pltpu
from jax.sharding import PartitionSpec as P

LATENT = 512
ROPE = 64
BLOCK = 64
LANES = 128
CHUNKS = LATENT // LANES
GRANT = 12 * 1024 * 1024
LAG_NS = 3500

score_scale = 1.0 / math.sqrt(192.0)
very_low = -1e30
f32 = jnp.float32
bf16 = jnp.bfloat16


def pieces(value):
    high = value.astype(bf16).astype(f32)
    rest = value - high
    middle = rest.astype(bf16).astype(f32)
    return high, middle, rest - middle


def spread_kernel(query_hbm, chosen_hbm, position_ref, out_ref, usable_ref, query_ref, chosen_ref, sems):
    copies = [
        pltpu.make_async_copy(source, target, sems.at[k])
        for k, (source, target) in enumerate(
            ((query_hbm, query_ref), (chosen_hbm, chosen_ref))
        )
    ]
    for copy in copies:
        copy.start()
    for copy in copies:
        copy.wait()
    steps, heads_dev, _ = query_ref.shape
    packed = []
    for t in range(steps):
        for c in range(CHUNKS):
            packed.append(query_ref[t, :, c * LANES : (c + 1) * LANES])
    rotary = [query_ref[t, :, LATENT:] for t in range(steps)]
    rotary.append(jnp.zeros_like(rotary[0]))
    for t in range(0, len(rotary), 2):
        packed.append(jnp.concatenate([rotary[t], rotary[t + 1]], axis=1))
    for k in range(0, len(packed), 2):
        tile = jnp.concatenate(packed[k : k + 2], axis=0)
        out_ref[:, k * heads_dev : (k + 2) * heads_dev, :] = jnp.broadcast_to(
            tile[None], (out_ref.shape[0], *tile.shape)
        )
    cache_len = usable_ref.shape[1]
    blocks = cache_len // BLOCK
    first = lax.axis_index("seq") * cache_len
    column = lax.broadcasted_iota(jnp.int32, (blocks, cache_len), 1)
    mine = column // BLOCK == lax.broadcasted_iota(jnp.int32, (blocks, cache_len), 0)
    mine = mine & (first + column < position_ref[0])
    wanted = chosen_ref.shape[2]
    block = first // BLOCK + lax.broadcasted_iota(jnp.int32, (blocks, wanted), 0)
    for t in range(steps):
        named = jnp.where(chosen_ref[t] == block, 1.0, 0.0)
        named = jnp.max(named, axis=1, keepdims=True)
        usable_ref[t : t + 1, :] = jnp.max(jnp.where(mine, named, 0.0), axis=0, keepdims=True)

    @pl.when(lax.axis_index("req") % 2 == 0)
    def _():
        pl.delay(LAG_NS)


def attend_kernel(usable_ref, query_ref, cache_ref, out_ref, rows_ref, rotary_ref, sums_ref, stats_ref):
    shards = query_ref.shape[0]
    steps = usable_ref.shape[0]
    heads = rotary_ref.shape[1]
    heads_dev = heads // shards
    for pair in range(rotary_ref.shape[0]):
        k = (steps * CHUNKS + pair) * heads_dev
        for s in range(shards):
            rotary_ref[pair, s * heads_dev : (s + 1) * heads_dev, :] = query_ref[s, k : k + heads_dev, :]
    for t in range(steps):
        for c in range(CHUNKS):
            k = (t * CHUNKS + c) * heads_dev
            for s in range(shards):
                row = t * heads + s * heads_dev
                rows_ref[row : row + heads_dev, c * LANES : (c + 1) * LANES] = query_ref[
                    s, k : k + heads_dev, :
                ]
    rotary = jnp.concatenate(
        [rotary_ref[t // 2, :, (t % 2) * ROPE : (t % 2 + 1) * ROPE] for t in range(steps)], axis=0
    )
    every = jnp.dot(rows_ref[...], cache_ref[:LATENT, :], preferred_element_type=f32)
    every = every + jnp.dot(rotary, cache_ref[LATENT:, :], preferred_element_type=f32)
    lane = lax.broadcasted_iota(jnp.int32, (heads, LANES), 1)
    slot = lane % (2 * steps)
    stats = jnp.zeros((heads, LANES), f32)
    weights = []
    for t in range(steps):
        scores = every[t * heads : (t + 1) * heads]
        scores = jnp.where(usable_ref[t : t + 1, :] > 0.0, scores, very_low)
        peak = jnp.max(scores, axis=1, keepdims=True)
        raw = jnp.exp2((scores - peak) * (score_scale * math.log2(math.e)))
        total = jnp.sum(raw, axis=1, keepdims=True)
        weights.append(raw.astype(bf16))
        stats = jnp.where(slot == 2 * t, peak * score_scale, stats)
        stats = jnp.where(slot == 2 * t + 1, total, stats)
    sums_ref[...] = lax.dot_general(
        jnp.concatenate(weights, axis=0),
        cache_ref[:LATENT, :],
        (((1,), (1,)), ((), ())),
        preferred_element_type=f32,
    ).astype(bf16)
    high, middle, low = pieces(stats)
    stats = jnp.where(lane < 2 * steps, high, jnp.where(lane < 4 * steps, middle, low))
    stats_ref[...] = stats.astype(bf16)
    for s in range(shards):
        for t in range(steps):
            row = t * heads + s * heads_dev
            for c in range(CHUNKS):
                out_ref[s, t * CHUNKS + c] = sums_ref[
                    row : row + heads_dev, c * LANES : (c + 1) * LANES
                ]
        out_ref[s, steps * CHUNKS] = stats_ref[s * heads_dev : (s + 1) * heads_dev, :]


def merge_kernel(parts_ref, value_ref, out_ref):
    shards, _, heads_dev, _ = parts_ref.shape
    requests, steps, _, _ = out_ref.shape
    stats = parts_ref[:, steps * CHUNKS].astype(f32)

    def shifted(value, by):
        return pltpu.roll(value, LANES - by, 2)

    stats = stats + shifted(stats, 2 * steps) + shifted(stats, 4 * steps)
    factors = jnp.exp(stats - jnp.max(stats, axis=0, keepdims=True))
    wholes = jnp.sum(shifted(stats, 1) * factors, axis=0)
    latent_out = []
    for t in range(steps):
        whole = wholes[:, 2 * t : 2 * t + 1]
        wide = jnp.broadcast_to(factors[:, :, 2 * t : 2 * t + 1], (shards, heads_dev, LANES))
        chunks = []
        for c in range(CHUNKS):
            part = parts_ref[:, t * CHUNKS + c].astype(f32)
            chunks.append(jnp.sum(part * wide, axis=0) / whole)
        latent_out.append(jnp.concatenate(chunks, axis=1))
    latent_out = jnp.concatenate(latent_out, axis=0).astype(bf16)
    row = lax.broadcasted_iota(jnp.int32, (steps * heads_dev, LANES), 0) % heads_dev
    every = jnp.dot(
        latent_out,
        jnp.concatenate([value_ref[h] for h in range(heads_dev)], axis=1),
        preferred_element_type=f32,
    )
    heads = every[:, :LANES]
    for h in range(1, heads_dev):
        heads = jnp.where(row == h, every[:, h * LANES : (h + 1) * LANES], heads)
    for t in range(steps):
        mine = heads[t * heads_dev : (t + 1) * heads_dev, :].astype(bf16)
        out_ref[:, t] = jnp.broadcast_to(mine[None], (requests, heads_dev, LANES))


def project_kernel(heads_ref, weight_ref, out_ref, flat_ref, wide_ref):
    requests, steps, heads_dev, _ = heads_ref.shape
    queries = requests * steps
    shards, half, width = out_ref.shape
    for q in range(queries):
        flat_ref[q * heads_dev : (q + 1) * heads_dev, :] = heads_ref[q // steps, q % steps]
    every = flat_ref[...]
    out_row = lax.broadcasted_iota(jnp.int32, (width, queries * heads_dev), 0)
    in_row = lax.broadcasted_iota(jnp.int32, (width, queries * heads_dev), 1)
    source = jnp.where(out_row < queries, out_row, out_row - queries) * heads_dev
    of_heads = []
    for h in range(heads_dev):
        pick = jnp.where(in_row == source + h, 1.0, 0.0).astype(bf16)
        of_heads.append(jnp.dot(pick, every, preferred_element_type=f32).astype(bf16))
    wide_ref[...] = lax.dot_general(
        weight_ref[...],
        jnp.concatenate(of_heads, axis=1),
        (((1,), (1,)), ((), ())),
        preferred_element_type=f32,
    )
    lane = lax.broadcasted_iota(jnp.int32, (half, width), 1)
    for s in range(shards):
        first = wide_ref[2 * half * s : 2 * half * s + half, :]
        second = wide_ref[2 * half * s + half : 2 * half * (s + 1), :]
        out_ref[s] = jnp.where(lane < queries, first, second).astype(bf16)


def finish_kernel(parts_ref, out_ref):
    _, half, width = parts_ref.shape
    total = jnp.sum(parts_ref[...].astype(f32), axis=0)
    out_ref[:half, :] = total[:, : width // 2].astype(bf16)
    out_ref[half:, :] = total[:, width // 2 :].astype(bf16)


def exchanged(value, axis):
    return lax.all_to_all(value, axis, 0, 0, tiled=True)


def kernel(fn, shape, name, scratch=(), dtype=bf16):
    return pl.pallas_call(
        fn,
        out_shape=jax.ShapeDtypeStruct(shape, dtype),
        scratch_shapes=[pltpu.VMEM(*s) for s in scratch],
        compiler_params=pltpu.CompilerParams(vmem_limit_bytes=GRANT),
        name=name,
    )


def body(latent_cache, queries, chosen, position, w_value, w_out):
    cache_len, key_width = latent_cache.shape[1:]
    _, steps, heads_dev, _ = queries.shape
    shards = lax.axis_size("seq")
    requests = lax.axis_size("req")
    heads = shards * heads_dev

    packed_rows = (steps * CHUNKS + (steps + 1) // 2) * heads_dev
    query_all, usable = pl.pallas_call(
        spread_kernel,
        out_shape=(
            jax.ShapeDtypeStruct((shards, packed_rows, LANES), bf16),
            jax.ShapeDtypeStruct((steps, cache_len), f32),
        ),
        in_specs=[pl.BlockSpec(memory_space=pltpu.HBM)] * 2
        + [pl.BlockSpec(memory_space=pltpu.SMEM)],
        scratch_shapes=[
            pltpu.VMEM((steps, heads_dev, key_width), bf16),
            pltpu.VMEM((steps, 1, chosen.shape[2]), jnp.int32),
            pltpu.SemaphoreType.DMA((2,)),
        ],
        compiler_params=pltpu.CompilerParams(vmem_limit_bytes=GRANT),
        name="spread",
    )(
        pltpu.with_memory_space_constraint(queries[0], pltpu.HBM),
        pltpu.with_memory_space_constraint(jnp.swapaxes(chosen, 0, 1), pltpu.HBM),
        position,
    )
    query_all = exchanged(query_all, "seq")
    parts = kernel(
        attend_kernel,
        (shards, steps * CHUNKS + 1, heads_dev, LANES),
        "attend",
        (
            ((steps * heads, LATENT), bf16),
            (((steps + 1) // 2, heads, LANES), bf16),
            ((steps * heads, LATENT), bf16),
            ((heads, LANES), bf16),
        ),
    )(usable, query_all, latent_cache[0].T)
    parts = exchanged(parts, "seq")
    head_out = kernel(merge_kernel, (requests, steps, heads_dev, w_value.shape[2]), "merge")(
        parts, w_value
    )
    head_out = exchanged(head_out, "req")
    features = w_out.shape[1]
    count = requests * steps
    mixed = kernel(
        project_kernel,
        (shards, features // shards // 2, 2 * count),
        "project",
        (((count * heads_dev, LANES), bf16), ((features, 2 * count), f32)),
    )(head_out, w_out.T)
    mixed = exchanged(mixed, "seq")
    return kernel(finish_kernel, (features // shards, count), "finish")(mixed)


def solution(mesh):
    return jax.shard_map(
        body,
        mesh=mesh,
        in_specs=(
            P("req", "seq", None),
            P("req", None, "seq", None),
            P("req", None, None),
            P("req"),
            P("seq", None, None),
            P("seq", "req"),
        ),
        out_specs=P(("req", "seq"), None),
        check_vma=False,
    )
```

```python
import math

import jax
import jax.numpy as jnp
from jax import lax
from jax.experimental import pallas as pl
from jax.experimental.pallas import tpu as pltpu
from jax.sharding import Mesh
from jax.sharding import PartitionSpec as P

LATENT = 512
ROPE = 64
BLOCK = 64
LANES = 128
CHUNKS = LATENT // LANES
GRANT = 12 * 1024 * 1024
LAG_NS = 3000
SEQ = ("z2", "z1", "z0", "x")
ORDER = ("z0", "x", "z1", "z2")

score_scale = 1.0 / math.sqrt(192.0)
very_low = -1e30
f32 = jnp.float32
bf16 = jnp.bfloat16


def pieces(value):
    high = value.astype(bf16).astype(f32)
    rest = value - high
    middle = rest.astype(bf16).astype(f32)
    return high, middle, rest - middle


def spread_kernel(query_hbm, chosen_hbm, position_ref, out_ref, usable_ref, query_ref, chosen_ref, sems):
    copies = [
        pltpu.make_async_copy(source, target, sems.at[k])
        for k, (source, target) in enumerate(
            ((query_hbm, query_ref), (chosen_hbm, chosen_ref))
        )
    ]
    for copy in copies:
        copy.start()
    for copy in copies:
        copy.wait()
    steps, heads_dev, _ = query_ref.shape
    packed = []
    for t in range(steps):
        for c in range(CHUNKS):
            packed.append(query_ref[t, :, c * LANES : (c + 1) * LANES])
    rotary = [query_ref[t, :, LATENT:] for t in range(steps)]
    rotary.append(jnp.zeros_like(rotary[0]))
    for t in range(0, len(rotary), 2):
        packed.append(jnp.concatenate([rotary[t], rotary[t + 1]], axis=1))
    for k in range(0, len(packed), 2):
        tile = jnp.concatenate(packed[k : k + 2], axis=0)
        out_ref[:, k * heads_dev : (k + 2) * heads_dev, :] = jnp.broadcast_to(
            tile[None], (out_ref.shape[0], *tile.shape)
        )
    cache_len = usable_ref.shape[1]
    blocks = cache_len // BLOCK
    first = lax.axis_index(SEQ) * cache_len
    column = lax.broadcasted_iota(jnp.int32, (blocks, cache_len), 1)
    mine = column // BLOCK == lax.broadcasted_iota(jnp.int32, (blocks, cache_len), 0)
    mine = mine & (first + column < position_ref[0])
    wanted = chosen_ref.shape[2]
    block = first // BLOCK + lax.broadcasted_iota(jnp.int32, (blocks, wanted), 0)
    for t in range(steps):
        named = jnp.where(chosen_ref[t] == block, 1.0, 0.0)
        named = jnp.max(named, axis=1, keepdims=True)
        usable_ref[t : t + 1, :] = jnp.max(jnp.where(mine, named, 0.0), axis=0, keepdims=True)

    @pl.when(lax.axis_index("req") % 2 == 0)
    def _():
        pl.delay(LAG_NS)


def attend_kernel(usable_ref, query_ref, cache_ref, out_ref, rows_ref, rotary_ref, sums_ref, stats_ref):
    shards = query_ref.shape[0]
    steps = usable_ref.shape[0]
    heads = rotary_ref.shape[1]
    heads_dev = heads // shards
    for pair in range(rotary_ref.shape[0]):
        k = (steps * CHUNKS + pair) * heads_dev
        for s in range(shards):
            rotary_ref[pair, s * heads_dev : (s + 1) * heads_dev, :] = query_ref[s, k : k + heads_dev, :]
    for t in range(steps):
        for c in range(CHUNKS):
            k = (t * CHUNKS + c) * heads_dev
            for s in range(shards):
                row = t * heads + s * heads_dev
                rows_ref[row : row + heads_dev, c * LANES : (c + 1) * LANES] = query_ref[
                    s, k : k + heads_dev, :
                ]
    rotary = jnp.concatenate(
        [rotary_ref[t // 2, :, (t % 2) * ROPE : (t % 2 + 1) * ROPE] for t in range(steps)], axis=0
    )
    every = jnp.dot(rows_ref[...], cache_ref[:LATENT, :], preferred_element_type=f32)
    every = every + jnp.dot(rotary, cache_ref[LATENT:, :], preferred_element_type=f32)
    lane = lax.broadcasted_iota(jnp.int32, (heads, LANES), 1)
    slot = lane % (2 * steps)
    stats = jnp.zeros((heads, LANES), f32)
    weights = []
    for t in range(steps):
        scores = every[t * heads : (t + 1) * heads]
        scores = jnp.where(usable_ref[t : t + 1, :] > 0.0, scores, very_low)
        peak = jnp.max(scores, axis=1, keepdims=True)
        raw = jnp.exp2((scores - peak) * (score_scale * math.log2(math.e)))
        total = jnp.sum(raw, axis=1, keepdims=True)
        weights.append(raw.astype(bf16))
        stats = jnp.where(slot == 2 * t, peak * score_scale, stats)
        stats = jnp.where(slot == 2 * t + 1, total, stats)
    sums_ref[...] = lax.dot_general(
        jnp.concatenate(weights, axis=0),
        cache_ref[:LATENT, :],
        (((1,), (1,)), ((), ())),
        preferred_element_type=f32,
    ).astype(bf16)
    high, middle, low = pieces(stats)
    stats = jnp.where(lane < 2 * steps, high, jnp.where(lane < 4 * steps, middle, low))
    stats_ref[...] = stats.astype(bf16)
    for s in range(shards):
        for t in range(steps):
            row = t * heads + s * heads_dev
            for c in range(CHUNKS):
                out_ref[s, t * CHUNKS + c] = sums_ref[
                    row : row + heads_dev, c * LANES : (c + 1) * LANES
                ]
        out_ref[s, steps * CHUNKS] = stats_ref[s * heads_dev : (s + 1) * heads_dev, :]


def merge_kernel(parts_ref, value_ref, out_ref):
    shards, _, heads_dev, _ = parts_ref.shape
    requests, steps, _, _ = out_ref.shape
    stats = parts_ref[:, steps * CHUNKS].astype(f32)

    def shifted(value, by):
        return pltpu.roll(value, LANES - by, 2)

    stats = stats + shifted(stats, 2 * steps) + shifted(stats, 4 * steps)
    factors = jnp.exp(stats - jnp.max(stats, axis=0, keepdims=True))
    wholes = jnp.sum(shifted(stats, 1) * factors, axis=0)
    latent_out = []
    for t in range(steps):
        whole = wholes[:, 2 * t : 2 * t + 1]
        wide = jnp.broadcast_to(factors[:, :, 2 * t : 2 * t + 1], (shards, heads_dev, LANES))
        chunks = []
        for c in range(CHUNKS):
            part = parts_ref[:, t * CHUNKS + c].astype(f32)
            chunks.append(jnp.sum(part * wide, axis=0) / whole)
        latent_out.append(jnp.concatenate(chunks, axis=1))
    latent_out = jnp.concatenate(latent_out, axis=0).astype(bf16)
    row = lax.broadcasted_iota(jnp.int32, (steps * heads_dev, LANES), 0) % heads_dev
    every = jnp.dot(
        latent_out,
        jnp.concatenate([value_ref[h] for h in range(heads_dev)], axis=1),
        preferred_element_type=f32,
    )
    heads = every[:, :LANES]
    for h in range(1, heads_dev):
        heads = jnp.where(row == h, every[:, h * LANES : (h + 1) * LANES], heads)
    for t in range(steps):
        mine = heads[t * heads_dev : (t + 1) * heads_dev, :].astype(bf16)
        out_ref[:, t] = jnp.broadcast_to(mine[None], (requests, heads_dev, LANES))


def project_kernel(heads_ref, weight_ref, out_ref, flat_ref, wide_ref):
    requests, steps, heads_dev, _ = heads_ref.shape
    queries = requests * steps
    shards, half, width = out_ref.shape
    for q in range(queries):
        flat_ref[q * heads_dev : (q + 1) * heads_dev, :] = heads_ref[q // steps, q % steps]
    every = flat_ref[...]
    out_row = lax.broadcasted_iota(jnp.int32, (width, queries * heads_dev), 0)
    in_row = lax.broadcasted_iota(jnp.int32, (width, queries * heads_dev), 1)
    source = jnp.where(out_row < queries, out_row, out_row - queries) * heads_dev
    of_heads = []
    for h in range(heads_dev):
        pick = jnp.where(in_row == source + h, 1.0, 0.0).astype(bf16)
        of_heads.append(jnp.dot(pick, every, preferred_element_type=f32).astype(bf16))
    wide_ref[...] = lax.dot_general(
        weight_ref[...],
        jnp.concatenate(of_heads, axis=1),
        (((1,), (1,)), ((), ())),
        preferred_element_type=f32,
    )
    lane = lax.broadcasted_iota(jnp.int32, (half, width), 1)
    for s in range(shards):
        first = wide_ref[2 * half * s : 2 * half * s + half, :]
        second = wide_ref[2 * half * s + half : 2 * half * (s + 1), :]
        out_ref[s] = jnp.where(lane < queries, first, second).astype(bf16)


def finish_kernel(parts_ref, out_ref):
    _, half, width = parts_ref.shape
    total = jnp.sum(parts_ref[...].astype(f32), axis=0)
    out_ref[:half, :] = total[:, : width // 2].astype(bf16)
    out_ref[half:, :] = total[:, width // 2 :].astype(bf16)


def exchanged(value, axis):
    return lax.all_to_all(value, axis, 0, 0, tiled=True)


def kernel(fn, shape, name, scratch=(), dtype=bf16):
    return pl.pallas_call(
        fn,
        out_shape=jax.ShapeDtypeStruct(shape, dtype),
        scratch_shapes=[pltpu.VMEM(*s) for s in scratch],
        compiler_params=pltpu.CompilerParams(vmem_limit_bytes=GRANT),
        name=name,
    )


def body(latent_cache, queries, chosen, position, w_value, w_out):
    cache_len, key_width = latent_cache.shape[1:]
    _, steps, heads_dev, _ = queries.shape
    shards = lax.axis_size(SEQ)
    requests = lax.axis_size("req")
    heads = shards * heads_dev

    packed_rows = (steps * CHUNKS + (steps + 1) // 2) * heads_dev
    query_all, usable = pl.pallas_call(
        spread_kernel,
        out_shape=(
            jax.ShapeDtypeStruct((shards, packed_rows, LANES), bf16),
            jax.ShapeDtypeStruct((steps, cache_len), f32),
        ),
        in_specs=[pl.BlockSpec(memory_space=pltpu.HBM)] * 2
        + [pl.BlockSpec(memory_space=pltpu.SMEM)],
        scratch_shapes=[
            pltpu.VMEM((steps, heads_dev, key_width), bf16),
            pltpu.VMEM((steps, 1, chosen.shape[2]), jnp.int32),
            pltpu.SemaphoreType.DMA((2,)),
        ],
        compiler_params=pltpu.CompilerParams(vmem_limit_bytes=GRANT),
        name="spread",
    )(
        pltpu.with_memory_space_constraint(queries[0], pltpu.HBM),
        pltpu.with_memory_space_constraint(jnp.swapaxes(chosen, 0, 1), pltpu.HBM),
        position,
    )
    query_all = exchanged(query_all, ORDER)
    parts = kernel(
        attend_kernel,
        (shards, steps * CHUNKS + 1, heads_dev, LANES),
        "attend",
        (
            ((steps * heads, LATENT), bf16),
            (((steps + 1) // 2, heads, LANES), bf16),
            ((steps * heads, LATENT), bf16),
            ((heads, LANES), bf16),
        ),
    )(usable, query_all, latent_cache[0].T)
    parts = exchanged(parts, ORDER)
    head_out = kernel(merge_kernel, (requests, steps, heads_dev, w_value.shape[2]), "merge")(
        parts, w_value
    )
    head_out = exchanged(head_out, "req")
    features = w_out.shape[1]
    count = requests * steps
    mixed = kernel(
        project_kernel,
        (shards, features // shards // 2, 2 * count),
        "project",
        (((count * heads_dev, LANES), bf16), ((features, 2 * count), f32)),
    )(head_out, w_out.T)
    mixed = exchanged(mixed, SEQ)
    return kernel(finish_kernel, (features // shards, count), "finish")(mixed)


def solution(mesh):
    requests, shards = mesh.devices.shape
    fine = Mesh(mesh.devices.reshape(requests, 2, 2, 2, shards // 8), ("req", *SEQ))
    return jax.shard_map(
        body,
        mesh=fine,
        in_specs=(
            P("req", SEQ, None),
            P("req", None, SEQ, None),
            P("req", None, None),
            P("req"),
            P(SEQ, None, None),
            P(SEQ, "req"),
        ),
        out_specs=P(("req", *SEQ), None),
        check_vma=False,
    )
```
